256 devices in a mesh: gx: 8 (over z), gy: 8 (over y, core), gz: 4 (over x).
Axes of the slice: x: 4, y: 4, z: 8, core: 2. Of those that a mesh axis runs over, the one named last changes fastest.
Arguments:
- density: float32 [64, 64, 512], P('gx', 'gy', 'gz'), may hold values from 0.5 to 2
- base_velocity: float32 [3, 64, 64, 512], P(None, 'gx', 'gy', 'gz'), may hold values from -0.4 to 0.4
- cells: int32 [3, 65536], P(None, ('gx', 'gy', 'gz')), may hold values from 0 to 511, as said below
- offsets: float32 [3, 65536], P(None, ('gx', 'gy', 'gz')), may hold values from 0 to 1
- target: float32 [3, 65536], P(None, ('gx', 'gy', 'gz')), may hold values from -0.4 to 0.4
- stiffness: float32 [65536], P(('gx', 'gy', 'gz')), may hold values from 0.01 to 0.1
- counts: int32 [256], P(('gx', 'gy', 'gz')), may hold values from 1 to 256, as said below
Outputs:
- forces: float32 [3, 65536], P(None, ('gx', 'gy', 'gz'))
The draws below stay inside these ranges and needn't reach their ends.
Inputs may be any that keep to these rules, and one draw needn't show every extreme that they name: `cells`: each marker's cell lies inside the lattice block of the device that holds its slot. `counts`: some device holds exactly 256 live markers in every draw.
All inputs are finite; a program needn't handle non-finite values.
Results may differ from the reference program's by a relative error of at most 0.0001.
Values sent between devices are 32-bit elements; how exact they have to be, the bound alone decides.
A program may use at most 64 MiB of HBM per device.

```python
import math
import jax
import jax.numpy as jnp
from jax import lax

CX = 8
CY = 8
CZ = 128
CAP = 256
ITERS = 3
NX = 64
NY = 64
NZ = 512
SLOTS = 65536
DEVICES = 256


def draw_cells(key, part):
    blocks_y = NY // CY
    blocks_z = NZ // CZ
    device = jnp.arange(SLOTS, dtype=jnp.int32) // CAP
    block_x = device // (blocks_y * blocks_z)
    block_y = device // blocks_z % blocks_y
    block_z = device % blocks_z
    keys = jax.random.split(key, 3)
    inside_x = jax.random.randint(keys[0], (SLOTS,), 0, CX, dtype=jnp.int32)
    inside_y = jax.random.randint(keys[1], (SLOTS,), 0, CY, dtype=jnp.int32)
    inside_z = jax.random.randint(keys[2], (SLOTS,), 0, CZ, dtype=jnp.int32)
    return jnp.stack([block_x * CX + inside_x, block_y * CY + inside_y, block_z * CZ + inside_z]).astype(jnp.int32)


def draw_counts(key, part):
    keys = jax.random.split(key, 3)
    divisor = 1 + jax.random.randint(keys[0], (DEVICES,), 0, 6, dtype=jnp.int32)
    jitter = jax.random.randint(keys[1], (DEVICES,), 0, CAP // 8 + 1, dtype=jnp.int32)
    loads = jnp.maximum(CAP // divisor - jitter, 1)
    fullest = jax.random.randint(keys[2], (), 0, DEVICES, dtype=jnp.int32)
    loads = jnp.where(jnp.arange(DEVICES, dtype=jnp.int32) == fullest, CAP, loads)
    return loads.astype(jnp.int32)


def levels(stream_key, extent, shards, low, largest):
    level, own = 1.0, jax.random.fold_in(stream_key, 6)
    for axis_at, blocks in shards:
        steps = jnp.exp(jax.random.uniform(jax.random.fold_in(own, axis_at), (blocks,), jnp.float32, low / len(shards), largest / len(shards)))
        level = level * jnp.repeat(steps, extent[axis_at] // blocks).reshape([-1 if axis == axis_at else 1 for axis in range(len(extent))])
    return level


def normal_values(stream_key, dims, scale, limit, shards=(), kind=jnp.bfloat16):
    values = scale * jax.random.normal(stream_key, dims, jnp.float32)
    if shards:
        values = values * levels(stream_key, dims, shards, -0.22, 0.18)
    return jnp.clip(values, -limit, limit).astype(kind)


def setup_inputs(seed: int = 0) -> dict:
    seeds = jax.random.split(jax.random.key(seed), 8)
    return {
        "density": jnp.clip(jnp.exp(math.log(2.0) - 1.3862944 * jax.random.uniform(seeds[0], (NX, NY, NZ), jnp.float32) ** levels(seeds[0], (NX, NY, NZ), ((0, 8), (1, 8), (2, 4)), -0.2, 0.2)), 0.5, 2.0),
        "base_velocity": normal_values(seeds[1], (3, NX, NY, NZ), 0.05, 0.4, ((1, 8), (2, 8), (3, 4)), jnp.float32),
        "cells": draw_cells(jax.random.fold_in(seeds[7], 71), 0),
        "offsets": jnp.clip(1.0 * jax.random.uniform(seeds[3], (3, SLOTS), jnp.float32) ** levels(seeds[3], (3, SLOTS), ((1, 256),), -0.2, 0.2), 0.0, 1.0),
        "target": normal_values(seeds[4], (3, SLOTS), 0.05, 0.4, ((1, 256),), jnp.float32),
        "stiffness": jnp.clip(jnp.exp(math.log(0.1) - 2.3025851 * jax.random.uniform(seeds[5], (SLOTS,), jnp.float32) ** levels(seeds[5], (SLOTS,), ((0, 256),), -0.2, 0.2)), 0.01, 0.1),
        "counts": draw_counts(jax.random.fold_in(seeds[7], 71), 0),
    }


def moving_directions():
    listing = []
    for along_x in (-1, 0, 1):
        for along_y in (-1, 0, 1):
            for along_z in (-1, 0, 1):
                order = abs(along_x) + abs(along_y) + abs(along_z)
                if order == 1:
                    listing.append((along_x, along_y, along_z, 1.0 / 18.0))
                elif order == 2:
                    listing.append((along_x, along_y, along_z, 1.0 / 36.0))
    return listing

def delta_weights(fraction):

    def inner(radius):
        return (3.0 - 2.0 * radius + jnp.sqrt(1.0 + 4.0 * radius - 4.0 * radius * radius)) / 8.0

    def outer(radius):
        return (5.0 - 2.0 * radius - jnp.sqrt(-7.0 + 12.0 * radius - 4.0 * radius * radius)) / 8.0
    return jnp.stack([outer(1.0 + fraction), inner(fraction), inner(1.0 - fraction), outer(2.0 - fraction)])

def reference(density, base_velocity, cells, offsets, target, stiffness, counts):
    live = (jnp.arange(CAP, dtype=jnp.int32)[None, :] < counts[:, None]).reshape(-1).astype(jnp.float32)
    scale = lax.rsqrt(density)
    weight_x = delta_weights(offsets[0])
    weight_y = delta_weights(offsets[1])
    weight_z = delta_weights(offsets[2])
    index_x = [((cells[0] + shift - 1) % NX).astype(jnp.int32) for shift in range(4)]
    index_y = [((cells[1] + shift - 1) % NY).astype(jnp.int32) for shift in range(4)]
    index_z = [((cells[2] + shift - 1) % NZ).astype(jnp.int32) for shift in range(4)]
    directions = moving_directions()

    def interpolate(field):
        total = jnp.zeros((3, SLOTS), jnp.float32)
        for first in range(4):
            for second in range(4):
                for third in range(4):
                    weight = weight_x[first] * weight_y[second] * weight_z[third]
                    total = total + field[:, index_x[first], index_y[second], index_z[third]] * weight
        return total

    def spread(vector):
        grid = jnp.zeros((3, NX, NY, NZ), jnp.float32)
        for first in range(4):
            for second in range(4):
                for third in range(4):
                    weight = weight_x[first] * weight_y[second] * weight_z[third]
                    grid = grid.at[:, index_x[first], index_y[second], index_z[third]].add(vector * weight)
        return grid

    def apply(vector):
        moved = scale * spread(vector)
        post = [jnp.zeros((NX, NY, NZ), jnp.float32) for component in range(3)]
        for along_x, along_y, along_z, share in directions:
            population = 3.0 * share * (along_x * moved[0] + along_y * moved[1] + along_z * moved[2])
            shifted = jnp.roll(population, (along_x, along_y, along_z), axis=(0, 1, 2))
            for component, along in enumerate((along_x, along_y, along_z)):
                if along != 0:
                    post[component] = post[component] + along * shifted
        velocity = scale * (moved + jnp.stack(post)) * 0.5
        return live * (interpolate(velocity) + stiffness * vector)
    right = live * (target - interpolate(base_velocity))
    solution = jnp.zeros_like(right)
    residual = right
    direction = right
    norm_now = jnp.sum(residual * residual)
    for step in range(ITERS):
        image = apply(direction)
        alpha = norm_now / jnp.sum(direction * image)
        solution = solution + alpha * direction
        residual = residual - alpha * image
        norm_next = jnp.sum(residual * residual)
        direction = residual + norm_next / norm_now * direction
        norm_now = norm_next
    return solution
```

```python
import functools
import itertools

import jax
import jax.numpy as jnp
from jax import lax
from jax.experimental import pallas as pl
from jax.experimental.pallas import tpu as pltpu
from jax.sharding import PartitionSpec as P

ITERS = 3
LOW, HIGH = 2, 3
MESH_ID = pl.DeviceIdType.MESH
AXES = ("gx", "gy", "gz")


def round_up(value, multiple):
    return -(-value // multiple) * multiple


def axis_groups(count):
    groups = {}
    for shift in (0, -1, 1):
        groups.setdefault(shift % count, []).append(shift)
    return list(groups.items())


def span(shifts, size):
    if shifts == [0]:
        return 1, size + 3
    if shifts == [-1]:
        return 0, 4
    if shifts == [1]:
        return size + 1, 4
    return 0, size + 5


def weights(fraction):
    root = jnp.sqrt(1.0 + 4.0 * fraction - 4.0 * fraction * fraction)
    near, far = 3.0 - 2.0 * fraction, 1.0 + 2.0 * fraction
    return ((near - root) / 8.0, (near + root) / 8.0, (far + root) / 8.0, (far - root) / 8.0)


def table(cell, four, shifts, size, first, rows):
    place = lax.broadcasted_iota(jnp.int32, (rows, cell.shape[1]), 0).astype(jnp.float32) + first
    total = None
    for shift in shifts:
        apart = place - (cell + (1.0 + shift * size))
        part = jnp.where(apart == 3.0, four[3], 0.0)
        for number in (2, 1, 0):
            part = jnp.where(apart == float(number), four[number], part)
        total = part if total is None else total + part
    return total


def split(value):
    high = value.astype(jnp.bfloat16)
    return high, (value - high.astype(jnp.float32)).astype(jnp.bfloat16)


def dot_nt(a, b):
    return lax.dot_general(a, b, (((1,), (1,)), ((), ())), preferred_element_type=jnp.float32)


def dot_nn(a, b):
    return lax.dot_general(a, b, (((1,), (0,)), ((), ())), preferred_element_type=jnp.float32)


def kernel(
    counts, sizes, density, velocity, cells_in, offsets_in, target_in, stiffness_in, count_in, out,
    block, cells_ref, offsets_ref, target_ref, stiffness_ref, count_ref,
    fields, xbuf, ybuf, zpack, zbuf, nbuf, fbuf, rbuf, sbuf, txy, thi, tlo, whi, wlo, grid,
    lsem, nsend, nrecv, rsend, rrecv, ssend, srecv, hsend, hrecv,
):
    size_x, size_y, size_z = sizes
    cap = cells_ref.shape[1]
    rows_y, lanes = fields.shape[2], fields.shape[3]
    assert 8 * (size_x + 5) <= size_z == lanes - size_z
    wide_x = size_x + 5
    groups = [axis_groups(count) for count in counts]
    slots = list(itertools.product(*[[offset for offset, _ in group] for group in groups]))
    me = [lax.axis_index(name) for name in AXES]
    sent = []

    def device(offset):
        return tuple(lax.rem(m + o, n) for m, o, n in zip(me, offset, counts))

    def negated(offset):
        return tuple((-o) % n for o, n in zip(offset, counts))

    near = [o for o in itertools.product([0], range(counts[1]), range(counts[2])) if any(o)]
    far = [(o, 0, 0) for o in range(1, counts[0])]
    peers = sorted({slot for slot in slots if any(slot)} | set(near) | set(far))
    loads = [
        pltpu.make_async_copy(source, destination, lsem.at[k])
        for k, (source, destination) in enumerate(
            [
                (cells_in, cells_ref),
                (offsets_in, offsets_ref),
                (density, block.at[3]),
                (velocity, block.at[pl.ds(0, 3)]),
                (target_in, target_ref),
                (stiffness_in, stiffness_ref),
                (count_in, count_ref),
            ]
        )
    ]
    for load in loads:
        load.start()
    barrier = pltpu.get_barrier_semaphore()
    for peer in peers:
        pl.semaphore_signal(barrier, inc=1, device_id=device(peer), device_id_type=MESH_ID)

    def neighbour_copy(turn, number):
        return pltpu.make_async_remote_copy(
            src_ref=fbuf.at[turn - 1, 0] if turn else nbuf.at[0],
            dst_ref=fbuf.at[turn - 1, number] if turn else nbuf.at[number],
            send_sem=nsend.at[turn, number - 1],
            recv_sem=nrecv.at[turn, number - 1],
            device_id=device(negated(slots[number])),
            device_id_type=MESH_ID,
        )

    def send_round(turn):
        for number in sorted(range(1, len(slots)), key=lambda k: (slots[k][0] == 0, k)):
            copy = neighbour_copy(turn, number)
            copy.start()
            sent.append(copy)

    def wait_round(turn, off_x):
        for number in range(1, len(slots)):
            if slots[number][0] == off_x:
                neighbour_copy(turn, number).wait_recv()

    def sum_copy(turn, stage, number):
        members, buffer, send, receive = ((near, rbuf, rsend, rrecv), (far, sbuf, ssend, srecv))[stage]
        return pltpu.make_async_remote_copy(
            src_ref=buffer.at[turn, 0],
            dst_ref=buffer.at[turn, number + 1],
            send_sem=send.at[turn, number],
            recv_sem=receive.at[turn, number],
            device_id=device(negated(members[number])),
            device_id_type=MESH_ID,
        )

    def away(offset):
        return -sum(min(o, n - o) for o, n in zip(offset, counts))

    def send_sum(turn, stage, value):
        members, buffer = ((near, rbuf), (far, sbuf))[stage]
        buffer[turn, 0] = value
        for number in sorted(range(len(members)), key=lambda k: (away(members[k]), k)):
            copy = sum_copy(turn, stage, number)
            copy.start()
            sent.append(copy)

    def wait_sum(turn, stage):
        members, buffer = ((near, rbuf), (far, sbuf))[stage]
        for number in sorted(range(len(members)), key=lambda k: (-away(members[k]), k)):
            sum_copy(turn, stage, number).wait_recv()
        return jnp.sum(buffer[turn], axis=0)

    def put(turn, vector):
        for c in range(3):
            for part in range(cap // 128):
                fbuf[turn - 1, 0, pl.ds(c * (cap // 128) + part, 1), :] = vector[
                    c : c + 1, part * 128 : part * 128 + 128
                ]

    def taken(turn, number, c):
        each = cap // 128
        return jnp.concatenate(
            [fbuf[turn - 1, number, pl.ds(c * each + part, 1), :] for part in range(each)], axis=1
        )

    offs_y = sorted({1 % counts[1], (-1) % counts[1]})
    offs_z = sorted({1 % counts[2], (-1) % counts[2]})

    def halo_copy(number, source, target, offset):
        return pltpu.make_async_remote_copy(
            src_ref=source,
            dst_ref=target,
            send_sem=hsend.at[number],
            recv_sem=hrecv.at[number],
            device_id=device(negated(offset)),
            device_id_type=MESH_ID,
        )

    def go(copies):
        for copy in copies:
            copy.start()
            sent.append(copy)

    low, high = pl.ds(0, LOW), pl.ds(LOW, HIGH)
    along_x = [
        halo_copy(0, block.at[:, pl.ds(size_x - LOW, LOW)], xbuf.at[:, low], (counts[0] - 1, 0, 0)),
        halo_copy(1, block.at[:, pl.ds(0, HIGH)], xbuf.at[:, high], (1, 0, 0)),
    ]
    along_y, relayed_y = [], []
    for k, off in enumerate(offs_y):
        here = (0, off, 0)
        along_y.append(halo_copy(2 + k, block, ybuf.at[k, :, pl.ds(LOW, size_x)], here))
        relayed_y.append(halo_copy(4 + k, xbuf.at[:, low], ybuf.at[k, :, low], here))
        relayed_y.append(
            halo_copy(6 + k, xbuf.at[:, high], ybuf.at[k, :, pl.ds(LOW + size_x, HIGH)], here)
        )
    along_z = [halo_copy(8 + k, zpack, zbuf.at[k], (0, 0, off)) for k, off in enumerate(offs_z)]

    def widen():
        for copy in along_y + relayed_y:
            copy.wait_recv()
        below = ybuf.at[offs_y.index((-1) % counts[1])]
        above = ybuf.at[offs_y.index(1 % counts[1])]
        lane = lax.broadcasted_iota(jnp.int32, (4, rows_y, size_z), 2)
        zero = jnp.zeros((4, rows_y - size_y - LOW - HIGH, size_z), jnp.float32)
        packed = jnp.zeros((4, rows_y, size_z), jnp.float32)
        for plane in range(wide_x):
            if plane < LOW:
                own = xbuf[:, plane]
            elif plane < LOW + size_x:
                own = block[:, plane - LOW]
            else:
                own = xbuf[:, plane - size_x]
            tall = jnp.concatenate(
                [below[:, plane][:, size_y - LOW :], own, above[:, plane][:, :HIGH], zero], axis=1
            )
            fields[:, plane, :, pl.ds(0, size_z)] = tall
            ends = jnp.where(lane < HIGH, tall, pltpu.roll(tall, LOW + HIGH, 2))
            at = 8 * plane
            inside = (lane >= at) & (lane < at + LOW + HIGH)
            packed = jnp.where(inside, pltpu.roll(ends, at, 2) if at else ends, packed)
        zpack[...] = packed
        go(along_z)
        for copy in along_z:
            copy.wait_recv()
        before = zbuf[offs_z.index((-1) % counts[2])]
        after = zbuf[offs_z.index(1 % counts[2])]
        for plane in range(wide_x):
            at = 8 * plane
            tall = pltpu.roll(fields[:, plane, :, pl.ds(0, size_z)], LOW, 2)
            first = pltpu.roll(before, (-(at + HIGH)) % size_z, 2)
            last = pltpu.roll(after, (LOW - at) % size_z, 2)
            fields[:, plane, :, pl.ds(0, size_z)] = jnp.where(lane < LOW, first, tall)
            tail = jnp.where(lane < LOW, tall, jnp.where(lane < LOW + HIGH, last, 0.0))
            fields[:, plane, :, pl.ds(size_z, lanes - size_z)] = tail

    def build(xi, yi, zi):
        number = slots.index((groups[0][xi][0], groups[1][yi][0], groups[2][zi][0]))
        info = nbuf[number]
        cells = [info[k : k + 1] for k in range(3)]
        fours = [weights(info[k + 3 : k + 4]) for k in range(3)]
        block = (yi * len(groups[2]) + zi) * cap
        start, planes = span(groups[0][xi][1], size_x)
        first = start // 8 * 8
        tall = round_up(start + planes - first, 8)
        tab_x = table(cells[0], fours[0], groups[0][xi][1], size_x, float(first), tall)
        tab_y = table(cells[1], fours[1], groups[1][yi][1], size_y, 0.0, rows_y)
        for plane in range(planes):
            at = start - first + plane
            txy[xi, pl.ds(plane * rows_y, rows_y), pl.ds(block, cap)] = tab_x[at : at + 1] * tab_y
        shifts = groups[2][zi][1]
        start, planes = span(shifts, size_z)
        first = start // 16 * 16
        tall = round_up(start + planes - first, 16)
        tab_z = table(cells[2], fours[2], shifts, size_z, float(first), tall)
        high, low = split(tab_z)
        for ref, part in ((thi, high), (tlo, low)):
            if first:
                ref[xi, pl.ds(0, first), pl.ds(block, cap)] = jnp.zeros((first, cap), jnp.bfloat16)
            ref[xi, pl.ds(first, tall), pl.ds(block, cap)] = part
            rest = lanes - first - tall
            if rest:
                ref[xi, pl.ds(first + tall, rest), pl.ds(block, cap)] = jnp.zeros(
                    (rest, cap), jnp.bfloat16
                )

    start_own, planes_own = span(groups[0][0][1], size_x)

    def interpolate(field):
        rows = planes_own * rows_y
        high, low = split(field.reshape(3 * rows, lanes))
        z_high, z_low = thi[0, :, pl.ds(0, cap)], tlo[0, :, pl.ds(0, cap)]
        part = dot_nn(high, z_high) + dot_nn(low, z_high) + dot_nn(high, z_low)
        plane = txy[0, pl.ds(0, rows), pl.ds(0, cap)]
        return jnp.concatenate(
            [
                jnp.sum(part[c * rows : (c + 1) * rows] * plane, axis=0, keepdims=True)
                for c in range(3)
            ],
            axis=0,
        )

    def spread(turn, polls):
        for xi, (off_x, shifts) in enumerate(groups[0]):
            start, planes = span(shifts, size_x)
            rows = planes * rows_y
            wait_round(turn, off_x)
            for yi, (off_y, _) in enumerate(groups[1]):
                for zi, (off_z, _) in enumerate(groups[2]):
                    number = slots.index((off_x, off_y, off_z))
                    block = (yi * len(groups[2]) + zi) * cap
                    plane = txy[xi, pl.ds(0, rows), pl.ds(block, cap)]
                    for c in range(3):
                        high, low = split(plane * taken(turn, number, c))
                        whi[pl.ds(c * rows, rows), pl.ds(block, cap)] = high
                        wlo[pl.ds(c * rows, rows), pl.ds(block, cap)] = low
            high, low = whi[pl.ds(0, 3 * rows), :], wlo[pl.ds(0, 3 * rows), :]
            part = dot_nt(high, thi[xi]) + dot_nt(low, thi[xi]) + dot_nt(high, tlo[xi])
            part = part.reshape(3, planes, rows_y, lanes)
            if xi == 0:
                if start > 0:
                    grid[:, pl.ds(0, start)] = jnp.zeros((3, start, rows_y, lanes), jnp.float32)
                rest = wide_x - start - planes
                if rest > 0:
                    grid[:, pl.ds(start + planes, rest)] = jnp.zeros(
                        (3, rest, rows_y, lanes), jnp.float32
                    )
                grid[:, pl.ds(start, planes)] = part
            else:
                grid[:, pl.ds(start, planes)] += part
            if polls:
                polls.pop(0)()

    def shifted(value, by, axis):
        return pltpu.roll(value, by % value.shape[axis], axis)

    def both(value, axis):
        return shifted(value, -1, axis), shifted(value, 1, axis)

    def add(value, axis):
        up, down = both(value, axis)
        return up + down

    def sub(value, axis):
        up, down = both(value, axis)
        return up - down

    def respond():
        scale = fields[3]
        mx, my, mz = (scale * grid[c] for c in range(3))
        slope_y, slope_z = sub(my, 1), sub(mz, 2)
        sum_x = 2.0 * mx + add(mx, 1) + add(mx, 2)
        slope = slope_y + slope_z
        px = sum_x[2:] + sum_x[:-2] + slope[2:] - slope[:-2]
        slope_x = mx[2:] - mx[:-2]
        sum_y = (2.0 * my + add(my, 2))[1:-1] + my[2:] + my[:-2]
        py = add(sum_y, 1) + sub(slope_x + slope_z[1:-1], 1)
        sum_z = (2.0 * mz + add(mz, 1))[1:-1] + mz[2:] + mz[:-2]
        pz = add(sum_z, 2) + sub(slope_x + slope_y[1:-1], 2)
        half = scale[1:-1] * 0.5
        return jnp.stack(
            [half * (m[1:-1] + p * (1.0 / 12.0)) for m, p in ((mx, px), (my, py), (mz, pz))]
        )

    def apply(turn, vector, polls=()):
        polls = list(polls)
        spread(turn, polls)
        field = respond()
        for poll in polls:
            poll()
        return live * (interpolate(field) + stiffness * vector)

    def partial_sums(residual, image):
        folded = []
        for other in (residual, image):
            row = jnp.sum(residual * other, axis=0, keepdims=True)
            total = row[:, :128]
            for at in range(128, cap, 128):
                total = total + row[:, at : at + 128]
            folded.append(total)
        return jnp.concatenate(folded, axis=0)

    def totals(tile):
        return (
            jnp.sum(tile[0:1], axis=1, keepdims=True),
            jnp.sum(tile[1:2], axis=1, keepdims=True),
        )

    loads[0].wait()
    loads[1].wait()
    for k, size in enumerate(sizes):
        nbuf[0, pl.ds(k, 1), :] = (cells_ref[pl.ds(k, 1), :] - me[k] * size).astype(jnp.float32)
    nbuf[0, pl.ds(3, 3), :] = offsets_ref[...]
    build(0, 0, 0)
    loads[2].wait()
    loads[3].wait()
    block[3] = lax.rsqrt(block[3])
    pl.semaphore_wait(barrier, len(peers))
    go(along_x + along_y)
    send_round(0)
    loads[4].wait()
    loads[5].wait()
    loads[6].wait()
    target, stiffness = target_ref[...], stiffness_ref[...]
    live = (lax.broadcasted_iota(jnp.int32, (1, cap), 1) < count_ref[0]).astype(jnp.float32)
    for copy in along_x:
        copy.wait_recv()
    go(relayed_y)
    for off_x, _ in groups[0]:
        wait_round(0, off_x)
    for xi, yi, zi in itertools.product(*[range(len(group)) for group in groups]):
        if (xi, yi, zi) != (0, 0, 0):
            build(xi, yi, zi)
    widen()
    base = live * (target - interpolate(fields[pl.ds(0, 3), pl.ds(1, size_x + 3)]))
    put(1, base)
    send_round(1)
    first = apply(1, base)
    put(2, first)
    send_round(2)
    send_sum(0, 0, partial_sums(base, first))
    second = apply(2, first, [lambda: send_sum(0, 1, wait_sum(0, 0))])
    put(3, second)
    send_round(3)
    norm, product = totals(wait_sum(0, 1))
    alpha = norm / product
    answer = alpha * base
    residual, image = base - alpha * first, first - alpha * second
    send_sum(1, 0, partial_sums(residual, image))
    third = apply(3, second, [lambda: send_sum(1, 1, wait_sum(1, 0))])
    again = second - alpha * third
    norm_before, alpha_before = norm, alpha
    norm, product = totals(wait_sum(1, 1))
    ratio = norm / norm_before
    alpha = norm / (product - ratio * norm / alpha_before)
    direction = residual + ratio * base
    answer = answer + alpha * direction
    residual, image = residual - alpha * (image + ratio * first), image - alpha * (again + ratio * second)
    send_sum(2, 0, partial_sums(residual, image))
    send_sum(2, 1, wait_sum(2, 0))
    norm_before, alpha_before = norm, alpha
    norm, product = totals(wait_sum(2, 1))
    ratio = norm / norm_before
    alpha = norm / (product - ratio * norm / alpha_before)
    out[...] = answer + alpha * (residual + ratio * direction)
    for copy in sent:
        copy.wait_send()


def body(mesh_counts, density, base_velocity, cells, offsets, target, stiffness, counts):
    sizes = density.shape
    size_x, size_y, size_z = sizes
    cap = cells.shape[1]
    rows_y, lanes = round_up(size_y + 5, 16), round_up(size_z + 5, 128)
    groups = [axis_groups(count) for count in mesh_counts]
    number = len(groups[0]) * len(groups[1]) * len(groups[2])
    width = len(groups[1]) * len(groups[2]) * cap
    tallest = max(span(shifts, size_x)[1] for _, shifts in groups[0])
    turns = ITERS + 1
    near, far = mesh_counts[1] * mesh_counts[2], mesh_counts[0]
    return pl.pallas_call(
        functools.partial(kernel, mesh_counts, sizes),
        out_shape=jax.ShapeDtypeStruct((3, cap), jnp.float32),
        in_specs=[pl.BlockSpec(memory_space=pltpu.HBM)] * 7,
        out_specs=pl.BlockSpec(memory_space=pltpu.VMEM),
        scratch_shapes=[
            pltpu.VMEM((4, size_x, size_y, size_z), jnp.float32),
            pltpu.VMEM((3, cap), jnp.int32),
            pltpu.VMEM((3, cap), jnp.float32),
            pltpu.VMEM((3, cap), jnp.float32),
            pltpu.VMEM((1, cap), jnp.float32),
            pltpu.SMEM((1,), jnp.int32),
            pltpu.VMEM((4, size_x + 5, rows_y, lanes), jnp.float32),
            pltpu.VMEM((4, LOW + HIGH, size_y, size_z), jnp.float32),
            pltpu.VMEM((2, 4, size_x + 5, size_y, size_z), jnp.float32),
            pltpu.VMEM((4, rows_y, size_z), jnp.float32),
            pltpu.VMEM((2, 4, rows_y, size_z), jnp.float32),
            pltpu.VMEM((number, 8, cap), jnp.float32),
            pltpu.VMEM((ITERS, number, 3 * (cap // 128), 128), jnp.float32),
            pltpu.VMEM((ITERS, near, 2, 128), jnp.float32),
            pltpu.VMEM((ITERS, far, 2, 128), jnp.float32),
            pltpu.VMEM((len(groups[0]), tallest * rows_y, width), jnp.float32),
            pltpu.VMEM((len(groups[0]), lanes, width), jnp.bfloat16),
            pltpu.VMEM((len(groups[0]), lanes, width), jnp.bfloat16),
            pltpu.VMEM((3 * tallest * rows_y, width), jnp.bfloat16),
            pltpu.VMEM((3 * tallest * rows_y, width), jnp.bfloat16),
            pltpu.VMEM((3, size_x + 5, rows_y, lanes), jnp.float32),
            pltpu.SemaphoreType.DMA((7,)),
            pltpu.SemaphoreType.DMA((turns, number - 1)),
            pltpu.SemaphoreType.DMA((turns, number - 1)),
            pltpu.SemaphoreType.DMA((ITERS, near - 1)),
            pltpu.SemaphoreType.DMA((ITERS, near - 1)),
            pltpu.SemaphoreType.DMA((ITERS, far - 1)),
            pltpu.SemaphoreType.DMA((ITERS, far - 1)),
            pltpu.SemaphoreType.DMA((10,)),
            pltpu.SemaphoreType.DMA((10,)),
        ],
        compiler_params=pltpu.CompilerParams(
            collective_id=0, has_side_effects=True, vmem_limit_bytes=60 * 1024 * 1024
        ),
    )(density, base_velocity, cells, offsets, target, stiffness[None], counts)


def solution(mesh):
    return jax.shard_map(
        functools.partial(body, tuple(mesh.shape[name] for name in AXES)),
        mesh=mesh,
        in_specs=(
            P("gx", "gy", "gz"),
            P(None, "gx", "gy", "gz"),
            P(None, ("gx", "gy", "gz")),
            P(None, ("gx", "gy", "gz")),
            P(None, ("gx", "gy", "gz")),
            P(("gx", "gy", "gz")),
            P(("gx", "gy", "gz")),
        ),
        out_specs=P(None, ("gx", "gy", "gz")),
        check_vma=False,
    )
```

```python
import functools
import itertools

import jax
import jax.numpy as jnp
from jax import lax
from jax.experimental import pallas as pl
from jax.experimental.pallas import tpu as pltpu
from jax.sharding import PartitionSpec as P

ITERS = 3
LOW, HIGH = 2, 3
WIDE, TALL, HALF = 13, 16, 8
STEPS = (0, -1, 1)
MESH_ID = pl.DeviceIdType.MESH
AXES = ("gx", "gy", "gz")


def round_up(value, multiple):
    return -(-value // multiple) * multiple


def span(shift, size):
    return {0: (1, size + 3), -1: (0, 4), 1: (size + 1, 4)}[shift]


def weights(fraction):
    root = jnp.sqrt(1.0 + 4.0 * fraction - 4.0 * fraction * fraction)
    near, far = 3.0 - 2.0 * fraction, 1.0 + 2.0 * fraction
    return ((near - root) / 8.0, (near + root) / 8.0, (far + root) / 8.0, (far - root) / 8.0)


def table(cell, four, shift, size, first, rows):
    place = lax.broadcasted_iota(jnp.int32, (rows, cell.shape[1]), 0).astype(jnp.float32) + first
    apart = place - (cell + (1.0 + shift * size))
    total = jnp.where(apart == 3.0, four[3], 0.0)
    for number in (2, 1, 0):
        total = jnp.where(apart == float(number), four[number], total)
    return total


def split(value):
    high = value.astype(jnp.bfloat16)
    return high, (value - high.astype(jnp.float32)).astype(jnp.bfloat16)


def dot_nt(a, b):
    return lax.dot_general(a, b, (((1,), (1,)), ((), ())), preferred_element_type=jnp.float32)


def dot_nn(a, b):
    return lax.dot_general(a, b, (((1,), (0,)), ((), ())), preferred_element_type=jnp.float32)


def patches():
    found, base = {}, 0
    for step_x, step_y in itertools.product(STEPS, STEPS):
        row, rows = {0: (0, TALL), -1: (0, HALF), 1: (HALF, HALF)}[step_y]
        start, planes = span(step_x, 8)
        if step_x == 0 and step_y:
            planes += 1
        found[step_x, step_y] = (start, planes, row, rows, base)
        base += planes * rows
    return found, base


PATCHES, PATCH_ROWS = patches()
FLAT = list(PATCHES)


def kernel(
    counts, sizes, density, velocity, cells_in, offsets_in, target_in, stiffness_in, count_in, out,
    block, cells_ref, offsets_ref, target_ref, stiffness_ref, count_ref,
    fields, xbuf, ylow, yhigh, below, above, zlow, zhigh, zbuf, nbuf, fbuf, rbuf, sbuf,
    txy, thi, tlo, azz, tzz, edge, grid,
    lsem, nsend, nrecv, rsend, rrecv, ssend, srecv, hsend, hrecv,
):
    size_x, size_y, size_z = sizes
    cap = cells_ref.shape[1]
    lanes = fields.shape[3]
    slots = list(itertools.product(STEPS, STEPS, STEPS))
    me = [lax.axis_index(name) for name in AXES]
    sent = []

    def device(offset):
        return tuple(lax.rem(m + (o % n), n) for m, o, n in zip(me, offset, counts))

    def negated(offset):
        return tuple(-o for o in offset)

    near = [o for o in itertools.product([0], range(counts[1]), range(counts[2])) if any(o)]
    far = [(o, 0, 0) for o in range(1, counts[0])]
    wrapped = {tuple(o % n for o, n in zip(slot, counts)) for slot in slots if any(slot)}
    peers = sorted(wrapped | set(near) | set(far))
    loads = [
        pltpu.make_async_copy(source, destination, lsem.at[k])
        for k, (source, destination) in enumerate(
            [
                (velocity, block.at[pl.ds(0, 3)]),
                (density, block.at[3]),
                (cells_in, cells_ref),
                (offsets_in, offsets_ref),
                (target_in, target_ref),
                (stiffness_in, stiffness_ref),
                (count_in, count_ref),
            ]
        )
    ]
    for load in loads:
        load.start()
    barrier = pltpu.get_barrier_semaphore()
    for peer in peers:
        pl.semaphore_signal(barrier, inc=1, device_id=device(peer), device_id_type=MESH_ID)

    def go(copies):
        for copy in copies:
            copy.start()
            sent.append(copy)

    def neighbour_copy(turn, number):
        return pltpu.make_async_remote_copy(
            src_ref=fbuf.at[turn - 1, 0] if turn else nbuf.at[0],
            dst_ref=fbuf.at[turn - 1, number] if turn else nbuf.at[number],
            send_sem=nsend.at[turn, number - 1],
            recv_sem=nrecv.at[turn, number - 1],
            device_id=device(negated(slots[number])),
            device_id_type=MESH_ID,
        )

    def send_round(turn):
        far_first = sorted(range(1, len(slots)), key=lambda k: (-sum(map(abs, slots[k])), k))
        go([neighbour_copy(turn, number) for number in far_first])

    def wait_round(turn):
        for number in range(1, len(slots)):
            neighbour_copy(turn, number).wait_recv()

    def sum_copy(turn, stage, number):
        members, buffer, send, receive = ((near, rbuf, rsend, rrecv), (far, sbuf, ssend, srecv))[stage]
        return pltpu.make_async_remote_copy(
            src_ref=buffer.at[turn, 0],
            dst_ref=buffer.at[turn, number + 1],
            send_sem=send.at[turn, number],
            recv_sem=receive.at[turn, number],
            device_id=device(negated(members[number])),
            device_id_type=MESH_ID,
        )

    def away(offset):
        return -sum(min(o, n - o) for o, n in zip(offset, counts))

    def send_sum(turn, stage, value):
        members, buffer = ((near, rbuf), (far, sbuf))[stage]
        buffer[turn, 0] = value
        ordered = sorted(range(len(members)), key=lambda k: (away(members[k]), k))
        go([sum_copy(turn, stage, number) for number in ordered])

    def wait_sum(turn, stage):
        members, buffer = ((near, rbuf), (far, sbuf))[stage]
        for number in sorted(range(len(members)), key=lambda k: (-away(members[k]), k)):
            sum_copy(turn, stage, number).wait_recv()
        return jnp.sum(buffer[turn], axis=0)

    def put(turn, vector):
        for c in range(3):
            for part in range(cap // 128):
                fbuf[turn - 1, 0, pl.ds(c * (cap // 128) + part, 1), :] = vector[
                    c : c + 1, part * 128 : part * 128 + 128
                ]

    def joined(ref, at, number, k):
        each = cap // 128
        return jnp.concatenate(
            [ref[at, number, pl.ds(k * each + part, 1), :] for part in range(each)], axis=1
        )

    def mark(number, k):
        each = cap // 128
        parts = [divmod(k * each + part, 4) for part in range(each)]
        return jnp.concatenate([nbuf[number, a, pl.ds(b, 1), :] for a, b in parts], axis=1)

    def halo_copy(number, source, target, step):
        return pltpu.make_async_remote_copy(
            src_ref=source,
            dst_ref=target,
            send_sem=hsend.at[number],
            recv_sem=hrecv.at[number],
            device_id=device(negated(step)),
            device_id_type=MESH_ID,
        )

    flows, scalars = [], []
    plane_of = {-1: (size_x - LOW, LOW, 0), 1: (0, HIGH, LOW)}
    low_of = {-1: (1, 1, 0), 0: (0, 2, 1), 1: (0, 1, 3)}
    high_of = {-1: (3, 1, 0), 0: (0, 4, 1), 1: (0, 2, 5)}
    for copies, part in ((flows, pl.ds(0, 3)), (scalars, pl.ds(3, 1))):
        for step_x, step_y in sorted(FLAT, key=lambda o: -abs(o[0]) - abs(o[1])):
            if step_y:
                source, target, where = (
                    (ylow, below, low_of) if step_y < 0 else (yhigh, above, high_of)
                )
            elif step_x:
                source, target, where = block, xbuf, plane_of
            else:
                continue
            first, many, at = where[step_x]
            copies.append(
                halo_copy(
                    len(flows) + len(scalars),
                    source.at[part, pl.ds(first, many)],
                    target.at[part, pl.ds(at, many)],
                    (step_x, step_y, 0),
                )
            )
    edges = []
    for k, (step_x, step_y) in sorted(enumerate(FLAT), key=lambda o: -abs(o[1][0]) - abs(o[1][1])):
        for side, step_z in enumerate((-1, 1)):
            edges.append(
                halo_copy(
                    len(flows) + len(scalars) + len(edges),
                    (zlow, zhigh)[side],
                    zbuf.at[side, k],
                    (step_x, step_y, step_z),
                )
            )

    lane = lax.broadcasted_iota(jnp.int32, (size_y, size_z), 1)
    row = lax.broadcasted_iota(jnp.int32, (size_y, size_z), 0)

    def turned(value, by, axis):
        by %= value.shape[axis]
        return pltpu.roll(value, by, axis) if by else value

    def pack():
        low = [jnp.zeros((size_y, size_z), jnp.float32)] * 2
        high = [jnp.zeros((size_y, size_z), jnp.float32)] * 2
        for c in range(4):
            tiles_low = [None] * 2
            tiles_high = [None] * 4
            for plane in range(size_x):
                own = block[c, plane]
                t, q = divmod(plane, 4)
                moved = turned(own, 2 * q - 6, 0)
                tiles_low[t] = moved if q == 0 else jnp.where(row // 2 == q, moved, tiles_low[t])
                t, q = divmod(plane, 2)
                moved = turned(own, 4 * q, 0)
                tiles_high[t] = moved if q == 0 else jnp.where(row // 4 == q, moved, tiles_high[t])
                at = c * size_x + plane
                chain = plane % 2
                low[chain] = jnp.where(
                    lane // 2 == at, turned(own, 2 * at - (size_z - LOW), 1), low[chain]
                )
                high[chain] = jnp.where(lane // 4 == at, turned(own, 4 * at, 1), high[chain])
            for t in range(2):
                ylow[c, t] = tiles_low[t]
            for t in range(4):
                yhigh[c, t] = tiles_high[t]
        zlow[...] = jnp.where(lane // 2 % 2 == 0, low[0], low[1])
        zhigh[...] = jnp.where(lane // 4 % 2 == 0, high[0], high[1])

    def tall_of(down, own, up):
        moved = turned(own, LOW, 0)
        return (
            jnp.where(row < LOW, down, moved),
            jnp.where(row < LOW, moved, up),
        )

    def widen(components, first):
        sides = {}
        for step_x in STEPS:
            for side in range(2):
                down, own, up = (zbuf[side, FLAT.index((step_x, step_y))] for step_y in (-1, 0, 1))
                sides[step_x, side] = tall_of(turned(down, LOW, 0), own, turned(up, LOW, 0))
        for plane in range(WIDE):
            if plane < LOW:
                step_x, x = -1, plane + size_x - LOW
            elif plane < LOW + size_x:
                step_x, x = 0, plane - LOW
            else:
                step_x, x = 1, plane - LOW - size_x
            for c in components:
                own = block[c, x] if step_x == 0 else xbuf[c, plane if step_x < 0 else plane - size_x]
                source, _, at = low_of[step_x]
                down = turned(below[c, at + x // 4 - source], -2 * (x % 4), 0)
                source, _, at = high_of[step_x]
                up = turned(above[c, at + x // 2 - source], LOW - 4 * (x % 2), 0)
                talls = tall_of(down, own, up)
                index = c * size_x + x
                for half in range(2):
                    moved = turned(talls[half], LOW, 1)
                    start = turned(sides[step_x, 0][half], -2 * index, 1)
                    end = turned(sides[step_x, 1][half], LOW - 4 * index, 1)
                    left = jnp.where(lane < LOW, start, moved)
                    right = jnp.where(lane < LOW, moved, jnp.where(lane < LOW + HIGH, end, first))
                    if half:
                        left = jnp.where(row < LOW + HIGH, left, first)
                        right = jnp.where(row < LOW + HIGH, right, first)
                    if c == 3:
                        left, right = lax.rsqrt(left), lax.rsqrt(right)
                    rows = pl.ds(half * size_y, size_y)
                    fields[c, plane, rows, pl.ds(0, size_z)] = left
                    fields[c, plane, rows, pl.ds(size_z, size_z)] = right

    def tables(step_x, step_y, step_z):
        number = slots.index((step_x, step_y, step_z))
        cells = [mark(number, k) for k in range(3)]
        fours = [weights(mark(number, k + 3)) for k in range(3)]
        start, planes, first_row, rows, base = PATCHES[step_x, step_y]
        first = start // 8 * 8
        tall = round_up(start + planes - first, 8)
        tab_x = table(cells[0], fours[0], step_x, size_x, float(first), tall)
        tab_y = table(cells[1], fours[1], step_y, size_y, float(first_row), rows)
        return cells[2], fours[2], [
            tab_x[start - first + plane : start - first + plane + 1] * tab_y for plane in range(planes)
        ]

    def build_main(step_x, step_y):
        cell, four, products = tables(step_x, step_y, 0)
        start, planes, first_row, rows, base = PATCHES[step_x, step_y]
        for plane, product in enumerate(products):
            txy[pl.ds(base + plane * rows, rows), :] = product
        k = FLAT.index((step_x, step_y))
        used = round_up(size_z + 5, 16)
        high, low = split(table(cell, four, 0, size_z, 0.0, used))
        for ref, part in ((thi, high), (tlo, low)):
            ref[k, pl.ds(0, used), :] = part
            ref[k, pl.ds(used, lanes - used), :] = jnp.zeros((lanes - used, cap), jnp.bfloat16)

    def build_side(step_x, step_y, side):
        cell, four, products = tables(step_x, step_y, (-1, 1)[side])
        start, planes, first_row, rows, base = PATCHES[step_x, step_y]
        many = planes * rows
        high, low = split(jnp.concatenate(products, axis=0))
        azz[side, pl.ds(2 * base, many), :] = high
        azz[side, pl.ds(2 * base + many, many), :] = low
        k = FLAT.index((step_x, step_y))
        tzz[side, k] = table(cell, four, (-1, 1)[side], size_z, float(side * size_z), 8)

    _, own_planes, _, _, _ = PATCHES[0, 0]
    own_rows = own_planes * TALL

    def interpolate(field):
        high, low = split(field.reshape(3 * own_rows, lanes))
        z_high, z_low = thi[0], tlo[0]
        part = dot_nn(high, z_high) + dot_nn(low, z_high) + dot_nn(high, z_low)
        plane = txy[pl.ds(0, own_rows), :]
        return jnp.concatenate(
            [
                jnp.sum(part[c * own_rows : (c + 1) * own_rows] * plane, axis=0, keepdims=True)
                for c in range(3)
            ],
            axis=0,
        )

    def spread_main(turn, step_x, step_y):
        start, planes, first_row, rows, base = PATCHES[step_x, step_y]
        number = slots.index((step_x, step_y, 0))
        k = FLAT.index((step_x, step_y))
        plane = txy[pl.ds(base, planes * rows), :]
        high, low = split(
            jnp.concatenate([plane * joined(fbuf, turn - 1, number, c) for c in range(3)], axis=0)
        )
        part = dot_nt(high, thi[k]) + dot_nt(low, thi[k]) + dot_nt(high, tlo[k])
        part = part.reshape(3, planes, rows, lanes)
        if number == 0:
            for edge_plane in (0, WIDE - 1):
                grid[:, edge_plane] = jnp.zeros((3, TALL, lanes), jnp.float32)
            grid[:, pl.ds(start, planes)] = part
        else:
            grid[:, pl.ds(start, planes), pl.ds(first_row, rows)] += part

    def spread_side(turn, step_x, step_y, side):
        start, planes, first_row, rows, base = PATCHES[step_x, step_y]
        number = slots.index((step_x, step_y, (-1, 1)[side]))
        k = FLAT.index((step_x, step_y))
        many = planes * rows
        tab = tzz[side, k]
        pieces = [tab * joined(fbuf, turn - 1, number, c) for c in range(3)]
        high, low = split(jnp.concatenate(pieces + [jnp.zeros_like(tab)], axis=0))
        part = dot_nt(
            azz[side, pl.ds(2 * base, 2 * many), :], jnp.concatenate([high, low], axis=0)
        )
        part = (part[:many] + part[many:]).reshape(planes, rows, 64)
        where = (side, pl.ds(start, planes), pl.ds(first_row, rows), pl.ds(0, 64))
        if (step_x, step_y) == (0, 0):
            edge[where] = part
        else:
            edge[where] += part

    def finish_sides():
        inside = lax.broadcasted_iota(jnp.int32, (WIDE, TALL, size_z), 2) < 8
        for side in range(2):
            both = edge[side]
            both = both + turned(both, -32, 2)
            for c in range(3):
                part = jnp.where(inside, turned(both, -8 * c, 2), 0.0)
                grid[c, :, :, pl.ds(side * size_z, size_z)] += part

    def spread_rest(turn, polls):
        wait_round(turn)
        for side in range(2):
            for edge_plane in (0, WIDE - 1):
                edge[side, edge_plane] = jnp.zeros((TALL, size_z), jnp.float32)
        for step_x, step_y in FLAT:
            if step_x or step_y:
                spread_main(turn, step_x, step_y)
        for poll in polls:
            poll()
        for side in range(2):
            for step_x, step_y in FLAT:
                spread_side(turn, step_x, step_y, side)
        finish_sides()

    def add(value, axis):
        return turned(value, -1, axis) + turned(value, 1, axis)

    def sub(value, axis):
        return turned(value, -1, axis) - turned(value, 1, axis)

    def respond():
        scale = fields[3]
        mx, my, mz = (scale * grid[c] for c in range(3))
        slope_y, slope_z = sub(my, 1), sub(mz, 2)
        sum_x = 2.0 * mx + add(mx, 1) + add(mx, 2)
        slope = slope_y + slope_z
        px = sum_x[2:] + sum_x[:-2] + slope[2:] - slope[:-2]
        slope_x = mx[2:] - mx[:-2]
        sum_y = (2.0 * my + add(my, 2))[1:-1] + my[2:] + my[:-2]
        py = add(sum_y, 1) + sub(slope_x + slope_z[1:-1], 1)
        sum_z = (2.0 * mz + add(mz, 1))[1:-1] + mz[2:] + mz[:-2]
        pz = add(sum_z, 2) + sub(slope_x + slope_y[1:-1], 2)
        half = scale[1:-1] * 0.5
        return jnp.stack(
            [half * (m[1:-1] + p * (1.0 / 12.0)) for m, p in ((mx, px), (my, py), (mz, pz))]
        )

    def apply(turn, vector, polls=()):
        spread_rest(turn, polls)
        return live * (interpolate(respond()) + stiffness * vector)

    def partial_sums(residual, image):
        folded = []
        for other in (residual, image):
            line = jnp.sum(residual * other, axis=0, keepdims=True)
            total = line[:, :128]
            for at in range(128, cap, 128):
                total = total + line[:, at : at + 128]
            folded.append(total)
        return jnp.concatenate(folded, axis=0)

    def totals(tile):
        return (
            jnp.sum(tile[0:1], axis=1, keepdims=True),
            jnp.sum(tile[1:2], axis=1, keepdims=True),
        )

    loads[0].wait()
    loads[1].wait()
    pack()
    loads[2].wait()
    loads[3].wait()
    each = cap // 128
    for k, size in enumerate(sizes):
        local = (cells_ref[pl.ds(k, 1), :] - me[k] * size).astype(jnp.float32)
        for values, at in ((local, k), (offsets_ref[pl.ds(k, 1), :], k + 3)):
            for part in range(each):
                a, b = divmod(at * each + part, 4)
                nbuf[0, a, pl.ds(b, 1), :] = values[:, part * 128 : part * 128 + 128]
    for load in loads[4:]:
        load.wait()
    pl.semaphore_wait(barrier, len(peers))
    go(flows)
    go(edges)
    send_round(0)
    go(scalars)
    target, stiffness = target_ref[...], stiffness_ref[...]
    live = (lax.broadcasted_iota(jnp.int32, (1, cap), 1) < count_ref[0]).astype(jnp.float32)
    build_main(0, 0)
    edge[...] = jnp.zeros_like(edge)
    for copy in flows + edges:
        copy.wait_recv()
    widen((0, 1, 2), 0.0)
    base = live * (target - interpolate(fields[pl.ds(0, 3), pl.ds(1, own_planes)]))
    put(1, base)
    send_round(1)
    spread_main(1, 0, 0)
    wait_round(0)
    for step_x, step_y in FLAT:
        if step_x or step_y:
            build_main(step_x, step_y)
        build_side(step_x, step_y, 0)
        build_side(step_x, step_y, 1)
    for copy in scalars:
        copy.wait_recv()
    widen((3,), 1.0)
    first = apply(1, base)
    put(2, first)
    send_round(2)
    send_sum(0, 0, partial_sums(base, first))
    spread_main(2, 0, 0)
    second = apply(2, first, [lambda: send_sum(0, 1, wait_sum(0, 0))])
    put(3, second)
    send_round(3)
    spread_main(3, 0, 0)
    norm, product = totals(wait_sum(0, 1))
    alpha = norm / product
    answer = alpha * base
    residual, image = base - alpha * first, first - alpha * second
    send_sum(1, 0, partial_sums(residual, image))
    third = apply(3, second, [lambda: send_sum(1, 1, wait_sum(1, 0))])
    again = second - alpha * third
    norm_before, alpha_before = norm, alpha
    norm, product = totals(wait_sum(1, 1))
    ratio = norm / norm_before
    alpha = norm / (product - ratio * norm / alpha_before)
    direction = residual + ratio * base
    answer = answer + alpha * direction
    residual, image = (
        residual - alpha * (image + ratio * first),
        image - alpha * (again + ratio * second),
    )
    send_sum(2, 0, partial_sums(residual, image))
    send_sum(2, 1, wait_sum(2, 0))
    norm_before, alpha_before = norm, alpha
    norm, product = totals(wait_sum(2, 1))
    ratio = norm / norm_before
    alpha = norm / (product - ratio * norm / alpha_before)
    out[...] = answer + alpha * (residual + ratio * direction)
    for copy in sent:
        copy.wait_send()


def body(mesh_counts, density, base_velocity, cells, offsets, target, stiffness, counts):
    sizes = density.shape
    size_x, size_y, size_z = sizes
    cap = cells.shape[1]
    assert sizes == (8, 8, 128) and min(mesh_counts) > 2
    lanes = 2 * size_z
    number, flat = 27, 9
    turns = ITERS + 1
    near, far = mesh_counts[1] * mesh_counts[2], mesh_counts[0]
    halos = 34
    return pl.pallas_call(
        functools.partial(kernel, mesh_counts, sizes),
        out_shape=jax.ShapeDtypeStruct((3, cap), jnp.float32),
        in_specs=[pl.BlockSpec(memory_space=pltpu.HBM)] * 7,
        out_specs=pl.BlockSpec(memory_space=pltpu.VMEM),
        scratch_shapes=[
            pltpu.VMEM((4, size_x, size_y, size_z), jnp.float32),
            pltpu.VMEM((3, cap), jnp.int32),
            pltpu.VMEM((3, cap), jnp.float32),
            pltpu.VMEM((3, cap), jnp.float32),
            pltpu.VMEM((1, cap), jnp.float32),
            pltpu.SMEM((1,), jnp.int32),
            pltpu.VMEM((4, WIDE, TALL, lanes), jnp.float32),
            pltpu.VMEM((4, LOW + HIGH, size_y, size_z), jnp.float32),
            pltpu.VMEM((4, 2, size_y, size_z), jnp.float32),
            pltpu.VMEM((4, 4, size_y, size_z), jnp.float32),
            pltpu.VMEM((4, 4, size_y, size_z), jnp.float32),
            pltpu.VMEM((4, 7, size_y, size_z), jnp.float32),
            pltpu.VMEM((size_y, size_z), jnp.float32),
            pltpu.VMEM((size_y, size_z), jnp.float32),
            pltpu.VMEM((2, flat, size_y, size_z), jnp.float32),
            pltpu.VMEM((number, 3 * (cap // 256), 4, 128), jnp.float32),
            pltpu.VMEM((ITERS, number, 3 * (cap // 128), 128), jnp.float32),
            pltpu.VMEM((ITERS, near, 2, 128), jnp.float32),
            pltpu.VMEM((ITERS, far, 2, 128), jnp.float32),
            pltpu.VMEM((PATCH_ROWS, cap), jnp.float32),
            pltpu.VMEM((flat, lanes, cap), jnp.bfloat16),
            pltpu.VMEM((flat, lanes, cap), jnp.bfloat16),
            pltpu.VMEM((2, 2 * PATCH_ROWS, cap), jnp.bfloat16),
            pltpu.VMEM((2, flat, 8, cap), jnp.float32),
            pltpu.VMEM((2, WIDE, TALL, size_z), jnp.float32),
            pltpu.VMEM((3, WIDE, TALL, lanes), jnp.float32),
            pltpu.SemaphoreType.DMA((7,)),
            pltpu.SemaphoreType.DMA((turns, number - 1)),
            pltpu.SemaphoreType.DMA((turns, number - 1)),
            pltpu.SemaphoreType.DMA((ITERS, near - 1)),
            pltpu.SemaphoreType.DMA((ITERS, near - 1)),
            pltpu.SemaphoreType.DMA((ITERS, far - 1)),
            pltpu.SemaphoreType.DMA((ITERS, far - 1)),
            pltpu.SemaphoreType.DMA((halos,)),
            pltpu.SemaphoreType.DMA((halos,)),
        ],
        compiler_params=pltpu.CompilerParams(
            collective_id=0, has_side_effects=True, vmem_limit_bytes=60 * 1024 * 1024
        ),
    )(density, base_velocity, cells, offsets, target, stiffness[None], counts)


def solution(mesh):
    return jax.shard_map(
        functools.partial(body, tuple(mesh.shape[name] for name in AXES)),
        mesh=mesh,
        in_specs=(
            P("gx", "gy", "gz"),
            P(None, "gx", "gy", "gz"),
            P(None, ("gx", "gy", "gz")),
            P(None, ("gx", "gy", "gz")),
            P(None, ("gx", "gy", "gz")),
            P(("gx", "gy", "gz")),
            P(("gx", "gy", "gz")),
        ),
        out_specs=P(None, ("gx", "gy", "gz")),
        check_vma=False,
    )
```

```python
import functools
import itertools

import jax
import jax.numpy as jnp
from jax import lax
from jax.experimental import pallas as pl
from jax.experimental.pallas import tpu as pltpu
from jax.sharding import PartitionSpec as P

ITERS = 3
LOW, HIGH = 2, 3
WIDE, TALL, HALF = 13, 16, 8
STEPS = (0, -1, 1)
MESH_ID = pl.DeviceIdType.MESH
AXES = ("gx", "gy", "gz")


def round_up(value, multiple):
    return -(-value // multiple) * multiple


def span(shift, size):
    return {0: (1, size + 3), -1: (0, 4), 1: (size + 1, 4)}[shift]


def weights(fraction):
    root = jnp.sqrt(1.0 + 4.0 * fraction - 4.0 * fraction * fraction)
    near, far = 3.0 - 2.0 * fraction, 1.0 + 2.0 * fraction
    return ((near - root) / 8.0, (near + root) / 8.0, (far + root) / 8.0, (far - root) / 8.0)


def table(cell, four, shift, size, first, rows):
    place = lax.broadcasted_iota(jnp.int32, (rows, cell.shape[1]), 0).astype(jnp.float32) + first
    apart = place - (cell + (1.0 + shift * size))
    total = jnp.where(apart == 3.0, four[3], 0.0)
    for number in (2, 1, 0):
        total = jnp.where(apart == float(number), four[number], total)
    return total


def split(value):
    high = value.astype(jnp.bfloat16)
    return high, (value - high.astype(jnp.float32)).astype(jnp.bfloat16)


def dot_nt(a, b):
    return lax.dot_general(a, b, (((1,), (1,)), ((), ())), preferred_element_type=jnp.float32)


def dot_nn(a, b):
    return lax.dot_general(a, b, (((1,), (0,)), ((), ())), preferred_element_type=jnp.float32)


def patches():
    found, base = {}, 0
    for step_x, step_y in itertools.product(STEPS, STEPS):
        row, rows = {0: (0, TALL), -1: (0, HALF), 1: (HALF, HALF)}[step_y]
        start, planes = span(step_x, 8)
        if step_x == 0 and step_y:
            planes += 1
        found[step_x, step_y] = (start, planes, row, rows, base)
        base += planes * rows
    return found, base


PATCHES, PATCH_ROWS = patches()
FLAT = list(PATCHES)


def kernel(
    counts, sizes, density, velocity, cells_in, offsets_in, target_in, stiffness_in, count_in, out,
    block, cells_ref, offsets_ref, target_ref, stiffness_ref, count_ref,
    fields, xbuf, ylow, yhigh, below, above, zlow, zhigh, zbuf, nbuf, fbuf, rbuf, sbuf,
    txy, thi, tlo, azz, tzz, edge, grid,
    lsem, nsend, nrecv, rsend, rrecv, ssend, srecv, hsend, hrecv,
):
    size_x, size_y, size_z = sizes
    cap = cells_ref.shape[1]
    lanes = fields.shape[3]
    slots = list(itertools.product(STEPS, STEPS, STEPS))
    me = [lax.axis_index(name) for name in AXES]
    sent = []

    def device(offset):
        return tuple(lax.rem(m + (o % n), n) for m, o, n in zip(me, offset, counts))

    def negated(offset):
        return tuple(-o for o in offset)

    near = [o for o in itertools.product([0], range(counts[1]), range(counts[2])) if any(o)]
    far = [(o, 0, 0) for o in range(1, counts[0])]
    wrapped = {tuple(o % n for o, n in zip(slot, counts)) for slot in slots if any(slot)}
    peers = sorted(wrapped | set(near) | set(far))
    loads = [
        pltpu.make_async_copy(source, destination, lsem.at[k])
        for k, (source, destination) in enumerate(
            [
                (velocity, block.at[pl.ds(0, 3)]),
                (density, block.at[3]),
                (cells_in, cells_ref),
                (offsets_in, offsets_ref),
                (target_in, target_ref),
                (stiffness_in, stiffness_ref),
                (count_in, count_ref),
            ]
        )
    ]
    for load in loads:
        load.start()
    barrier = pltpu.get_barrier_semaphore()
    for peer in peers:
        pl.semaphore_signal(barrier, inc=1, device_id=device(peer), device_id_type=MESH_ID)

    def go(copies):
        for copy in copies:
            copy.start()

    def every(ref, send, receive):
        copy = pltpu.make_async_remote_copy(
            src_ref=ref,
            dst_ref=ref,
            send_sem=send,
            recv_sem=receive,
            device_id=device(far[0]),
            device_id_type=MESH_ID,
        )
        sent.append(copy)
        return copy

    def neighbour_copy(turn, number):
        return pltpu.make_async_remote_copy(
            src_ref=fbuf.at[turn - 1, 0] if turn else nbuf.at[0],
            dst_ref=fbuf.at[turn - 1, number] if turn else nbuf.at[number],
            send_sem=nsend.at[turn],
            recv_sem=nrecv.at[turn],
            device_id=device(negated(slots[number])),
            device_id_type=MESH_ID,
        )

    def send_round(turn):
        far_first = sorted(range(1, len(slots)), key=lambda k: (-sum(map(abs, slots[k])), k))
        go([neighbour_copy(turn, number) for number in far_first])

    def wait_round(turn):
        others = pl.ds(1, len(slots) - 1)
        landed = fbuf.at[turn - 1, others] if turn else nbuf.at[others]
        every(landed, nsend.at[turn], nrecv.at[turn]).wait_recv()

    def sum_copy(turn, stage, number):
        members, buffer, send, receive = ((near, rbuf, rsend, rrecv), (far, sbuf, ssend, srecv))[stage]
        return pltpu.make_async_remote_copy(
            src_ref=buffer.at[turn, 0],
            dst_ref=buffer.at[turn, number + 1],
            send_sem=send.at[turn],
            recv_sem=receive.at[turn],
            device_id=device(negated(members[number])),
            device_id_type=MESH_ID,
        )

    def away(offset):
        return -sum(min(o, n - o) for o, n in zip(offset, counts))

    def send_sum(turn, stage, value):
        members, buffer = ((near, rbuf), (far, sbuf))[stage]
        buffer[turn, 0] = value
        ordered = sorted(range(len(members)), key=lambda k: (away(members[k]), k))
        go([sum_copy(turn, stage, number) for number in ordered])

    def wait_sum(turn, stage):
        members, buffer, send, receive = ((near, rbuf, rsend, rrecv), (far, sbuf, ssend, srecv))[stage]
        every(buffer.at[turn, pl.ds(1, len(members))], send.at[turn], receive.at[turn]).wait_recv()
        return jnp.sum(buffer[turn], axis=0)

    def put(turn, vector):
        for c in range(3):
            for part in range(cap // 128):
                fbuf[turn - 1, 0, c, pl.ds(part, 1), :] = vector[
                    c : c + 1, part * 128 : part * 128 + 128
                ]

    def joined(ref, at, number, k):
        return jnp.concatenate(
            [ref[at, number, k, pl.ds(part, 1), :] for part in range(cap // 128)], axis=1
        )

    def mark(number, k):
        each = cap // 128
        parts = [divmod(k * each + part, 4) for part in range(each)]
        return jnp.concatenate([nbuf[number, a, pl.ds(b, 1), :] for a, b in parts], axis=1)

    def halo_copy(number, source, target, step):
        return pltpu.make_async_remote_copy(
            src_ref=source,
            dst_ref=target,
            send_sem=hsend.at[number],
            recv_sem=hrecv.at[number],
            device_id=device(negated(step)),
            device_id_type=MESH_ID,
        )

    flows, scalars, edges = [], [], []
    plane_of = {-1: (size_x - LOW, LOW, 0), 1: (0, HIGH, LOW)}
    low_of = {-1: (1, 1, 0), 0: (0, 2, 1), 1: (0, 1, 3)}
    high_of = {-1: (3, 1, 0), 0: (0, 4, 1), 1: (0, 2, 5)}
    spaces = ((block, xbuf, plane_of), (ylow, below, low_of), (yhigh, above, high_of))
    corners_first = sorted(FLAT, key=lambda o: -abs(o[0]) - abs(o[1]))
    halves = (pl.ds(0, 3), pl.ds(3, 1))
    for kind, copies in enumerate((flows, scalars)):
        for step_x, step_y in corners_first:
            if step_x == step_y == 0:
                continue
            space = 0 if step_y == 0 else 1 if step_y < 0 else 2
            source, target, where = spaces[space]
            first, many, at = where[step_x]
            copies.append(
                halo_copy(
                    3 * kind + space,
                    source.at[halves[kind], pl.ds(first, many)],
                    target.at[halves[kind], pl.ds(at, many)],
                    (step_x, step_y, 0),
                )
            )
    for step_x, step_y in corners_first:
        for side, step_z in enumerate((-1, 1)):
            edges.append(
                halo_copy(
                    6,
                    (zlow, zhigh)[side],
                    zbuf.at[side, FLAT.index((step_x, step_y))],
                    (step_x, step_y, step_z),
                )
            )

    def wait_halos(kind):
        for space, (_, target, _) in enumerate(spaces):
            at = 3 * kind + space
            every(target.at[halves[kind]], hsend.at[at], hrecv.at[at]).wait_recv()
        if kind == 0:
            every(zbuf, hsend.at[6], hrecv.at[6]).wait_recv()

    lane = lax.broadcasted_iota(jnp.int32, (size_y, size_z), 1)
    row = lax.broadcasted_iota(jnp.int32, (size_y, size_z), 0)

    def turned(value, by, axis):
        by %= value.shape[axis]
        return pltpu.roll(value, by, axis) if by else value

    def pack():
        low = [jnp.zeros((size_y, size_z), jnp.float32)] * 2
        high = [jnp.zeros((size_y, size_z), jnp.float32)] * 2
        for c in range(4):
            tiles_low = [None] * 2
            tiles_high = [None] * 4
            for plane in range(size_x):
                own = block[c, plane]
                t, q = divmod(plane, 4)
                moved = turned(own, 2 * q - 6, 0)
                tiles_low[t] = moved if q == 0 else jnp.where(row // 2 == q, moved, tiles_low[t])
                t, q = divmod(plane, 2)
                moved = turned(own, 4 * q, 0)
                tiles_high[t] = moved if q == 0 else jnp.where(row // 4 == q, moved, tiles_high[t])
                at = c * size_x + plane
                chain = plane % 2
                low[chain] = jnp.where(
                    lane // 2 == at, turned(own, 2 * at - (size_z - LOW), 1), low[chain]
                )
                high[chain] = jnp.where(lane // 4 == at, turned(own, 4 * at, 1), high[chain])
            for t in range(2):
                ylow[c, t] = tiles_low[t]
            for t in range(4):
                yhigh[c, t] = tiles_high[t]
        zlow[...] = jnp.where(lane // 2 % 2 == 0, low[0], low[1])
        zhigh[...] = jnp.where(lane // 4 % 2 == 0, high[0], high[1])

    def tall_of(down, own, up):
        moved = turned(own, LOW, 0)
        return (
            jnp.where(row < LOW, down, moved),
            jnp.where(row < LOW, moved, up),
        )

    def widen(components, first):
        sides = {}
        for step_x in STEPS:
            for side in range(2):
                down, own, up = (zbuf[side, FLAT.index((step_x, step_y))] for step_y in (-1, 0, 1))
                sides[step_x, side] = tall_of(turned(down, LOW, 0), own, turned(up, LOW, 0))
        for plane in range(WIDE):
            if plane < LOW:
                step_x, x = -1, plane + size_x - LOW
            elif plane < LOW + size_x:
                step_x, x = 0, plane - LOW
            else:
                step_x, x = 1, plane - LOW - size_x
            for c in components:
                own = block[c, x] if step_x == 0 else xbuf[c, plane if step_x < 0 else plane - size_x]
                source, _, at = low_of[step_x]
                down = turned(below[c, at + x // 4 - source], -2 * (x % 4), 0)
                source, _, at = high_of[step_x]
                up = turned(above[c, at + x // 2 - source], LOW - 4 * (x % 2), 0)
                talls = tall_of(down, own, up)
                index = c * size_x + x
                for half in range(2):
                    moved = turned(talls[half], LOW, 1)
                    start = turned(sides[step_x, 0][half], -2 * index, 1)
                    end = turned(sides[step_x, 1][half], LOW - 4 * index, 1)
                    left = jnp.where(lane < LOW, start, moved)
                    right = jnp.where(lane < LOW, moved, jnp.where(lane < LOW + HIGH, end, first))
                    if half:
                        left = jnp.where(row < LOW + HIGH, left, first)
                        right = jnp.where(row < LOW + HIGH, right, first)
                    if c == 3:
                        left, right = lax.rsqrt(left), lax.rsqrt(right)
                    rows = pl.ds(half * size_y, size_y)
                    fields[c, plane, rows, pl.ds(0, size_z)] = left
                    fields[c, plane, rows, pl.ds(size_z, size_z)] = right

    def tables(step_x, step_y, step_z):
        number = slots.index((step_x, step_y, step_z))
        cells = [mark(number, k) for k in range(3)]
        fours = [weights(mark(number, k + 3)) for k in range(3)]
        start, planes, first_row, rows, base = PATCHES[step_x, step_y]
        first = start // 8 * 8
        tall = round_up(start + planes - first, 8)
        tab_x = table(cells[0], fours[0], step_x, size_x, float(first), tall)
        tab_y = table(cells[1], fours[1], step_y, size_y, float(first_row), rows)
        return cells[2], fours[2], [
            tab_x[start - first + plane : start - first + plane + 1] * tab_y for plane in range(planes)
        ]

    def build_main(step_x, step_y):
        cell, four, products = tables(step_x, step_y, 0)
        start, planes, first_row, rows, base = PATCHES[step_x, step_y]
        for plane, product in enumerate(products):
            txy[pl.ds(base + plane * rows, rows), :] = product
        k = FLAT.index((step_x, step_y))
        used = round_up(size_z + 5, 16)
        high, low = split(table(cell, four, 0, size_z, 0.0, used))
        for ref, part in ((thi, high), (tlo, low)):
            ref[k, pl.ds(0, used), :] = part
            ref[k, pl.ds(used, lanes - used), :] = jnp.zeros((lanes - used, cap), jnp.bfloat16)

    def build_side(step_x, step_y, side):
        cell, four, products = tables(step_x, step_y, (-1, 1)[side])
        start, planes, first_row, rows, base = PATCHES[step_x, step_y]
        many = planes * rows
        high, low = split(jnp.concatenate(products, axis=0))
        azz[side, pl.ds(2 * base, many), :] = high
        azz[side, pl.ds(2 * base + many, many), :] = low
        k = FLAT.index((step_x, step_y))
        tzz[side, k] = table(cell, four, (-1, 1)[side], size_z, float(side * size_z), 8)

    _, own_planes, _, _, _ = PATCHES[0, 0]
    own_rows = own_planes * TALL

    def interpolate(field):
        high, low = split(field.reshape(3 * own_rows, lanes))
        z_high, z_low = thi[0], tlo[0]
        part = dot_nn(high, z_high) + dot_nn(low, z_high) + dot_nn(high, z_low)
        plane = txy[pl.ds(0, own_rows), :]
        return jnp.concatenate(
            [
                jnp.sum(part[c * own_rows : (c + 1) * own_rows] * plane, axis=0, keepdims=True)
                for c in range(3)
            ],
            axis=0,
        )

    def spread_main(turn, step_x, step_y):
        start, planes, first_row, rows, base = PATCHES[step_x, step_y]
        number = slots.index((step_x, step_y, 0))
        k = FLAT.index((step_x, step_y))
        plane = txy[pl.ds(base, planes * rows), :]
        high, low = split(
            jnp.concatenate([plane * joined(fbuf, turn - 1, number, c) for c in range(3)], axis=0)
        )
        part = dot_nt(high, thi[k]) + dot_nt(low, thi[k]) + dot_nt(high, tlo[k])
        part = part.reshape(3, planes, rows, lanes)
        if number == 0:
            for edge_plane in (0, WIDE - 1):
                grid[:, edge_plane] = jnp.zeros((3, TALL, lanes), jnp.float32)
            grid[:, pl.ds(start, planes)] = part
        else:
            grid[:, pl.ds(start, planes), pl.ds(first_row, rows)] += part

    def spread_side(turn, step_x, step_y, side):
        start, planes, first_row, rows, base = PATCHES[step_x, step_y]
        number = slots.index((step_x, step_y, (-1, 1)[side]))
        k = FLAT.index((step_x, step_y))
        many = planes * rows
        tab = tzz[side, k]
        pieces = [tab * joined(fbuf, turn - 1, number, c) for c in range(3)]
        high, low = split(jnp.concatenate(pieces + [jnp.zeros_like(tab)], axis=0))
        part = dot_nt(
            azz[side, pl.ds(2 * base, 2 * many), :], jnp.concatenate([high, low], axis=0)
        )
        part = (part[:many] + part[many:]).reshape(planes, rows, 64)
        where = (side, pl.ds(start, planes), pl.ds(first_row, rows), pl.ds(0, 64))
        if (step_x, step_y) == (0, 0):
            edge[where] = part
        else:
            edge[where] += part

    def finish_sides():
        inside = lax.broadcasted_iota(jnp.int32, (WIDE, TALL, size_z), 2) < 8
        for side in range(2):
            both = edge[side]
            both = both + turned(both, -32, 2)
            for c in range(3):
                part = jnp.where(inside, turned(both, -8 * c, 2), 0.0)
                grid[c, :, :, pl.ds(side * size_z, size_z)] += part

    def spread_rest(turn, early, late):
        wait_round(turn)
        if early:
            early()
        for side in range(2):
            for edge_plane in (0, WIDE - 1):
                edge[side, edge_plane] = jnp.zeros((TALL, size_z), jnp.float32)
        for step_x, step_y in FLAT:
            if step_x or step_y:
                spread_main(turn, step_x, step_y)
        if late:
            late()
        for side in range(2):
            for step_x, step_y in FLAT:
                spread_side(turn, step_x, step_y, side)
        finish_sides()

    def add(value, axis):
        return turned(value, -1, axis) + turned(value, 1, axis)

    def sub(value, axis):
        return turned(value, -1, axis) - turned(value, 1, axis)

    def respond():
        scale = fields[3]
        mx, my, mz = (scale * grid[c] for c in range(3))
        slope_y, slope_z = sub(my, 1), sub(mz, 2)
        sum_x = 2.0 * mx + add(mx, 1) + add(mx, 2)
        slope = slope_y + slope_z
        px = sum_x[2:] + sum_x[:-2] + slope[2:] - slope[:-2]
        slope_x = mx[2:] - mx[:-2]
        sum_y = (2.0 * my + add(my, 2))[1:-1] + my[2:] + my[:-2]
        py = add(sum_y, 1) + sub(slope_x + slope_z[1:-1], 1)
        sum_z = (2.0 * mz + add(mz, 1))[1:-1] + mz[2:] + mz[:-2]
        pz = add(sum_z, 2) + sub(slope_x + slope_y[1:-1], 2)
        half = scale[1:-1] * 0.5
        return jnp.stack(
            [half * (m[1:-1] + p * (1.0 / 12.0)) for m, p in ((mx, px), (my, py), (mz, pz))]
        )

    def apply(turn, vector, early=None, late=None):
        spread_rest(turn, early, late)
        return live * (interpolate(respond()) + stiffness * vector)

    def partial_sums(residual, image):
        folded = []
        for other in (residual, image):
            line = jnp.sum(residual * other, axis=0, keepdims=True)
            total = line[:, :128]
            for at in range(128, cap, 128):
                total = total + line[:, at : at + 128]
            folded.append(total)
        return jnp.concatenate(folded, axis=0)

    def totals(tile):
        return (
            jnp.sum(tile[0:1], axis=1, keepdims=True),
            jnp.sum(tile[1:2], axis=1, keepdims=True),
        )

    loads[0].wait()
    loads[1].wait()
    pack()
    loads[2].wait()
    loads[3].wait()
    each = cap // 128
    for k, size in enumerate(sizes):
        local = (cells_ref[pl.ds(k, 1), :] - me[k] * size).astype(jnp.float32)
        for values, at in ((local, k), (offsets_ref[pl.ds(k, 1), :], k + 3)):
            for part in range(each):
                a, b = divmod(at * each + part, 4)
                nbuf[0, a, pl.ds(b, 1), :] = values[:, part * 128 : part * 128 + 128]
    for load in loads[4:]:
        load.wait()
    pl.semaphore_wait(barrier, len(peers))
    go(flows)
    go(edges)
    send_round(0)
    go(scalars)
    target, stiffness = target_ref[...], stiffness_ref[...]
    live = (lax.broadcasted_iota(jnp.int32, (1, cap), 1) < count_ref[0]).astype(jnp.float32)
    build_main(0, 0)
    edge[...] = jnp.zeros_like(edge)
    wait_halos(0)
    widen((0, 1, 2), 0.0)
    base = live * (target - interpolate(fields[pl.ds(0, 3), pl.ds(1, own_planes)]))
    put(1, base)
    send_round(1)
    spread_main(1, 0, 0)
    wait_round(0)
    for step_x, step_y in FLAT:
        if step_x or step_y:
            build_main(step_x, step_y)
        build_side(step_x, step_y, 0)
        build_side(step_x, step_y, 1)
    wait_halos(1)
    widen((3,), 1.0)
    first = apply(1, base)
    put(2, first)
    send_round(2)
    send_sum(0, 0, partial_sums(base, first))
    spread_main(2, 0, 0)
    second = apply(2, first, early=lambda: send_sum(0, 1, wait_sum(0, 0)))
    put(3, second)
    send_round(3)
    spread_main(3, 0, 0)
    norm, product = totals(wait_sum(0, 1))
    alpha = norm / product
    answer = alpha * base
    residual, image = base - alpha * first, first - alpha * second
    send_sum(1, 0, partial_sums(residual, image))
    third = apply(3, second, late=lambda: send_sum(1, 1, wait_sum(1, 0)))
    again = second - alpha * third
    norm_before, alpha_before = norm, alpha
    norm, product = totals(wait_sum(1, 1))
    ratio = norm / norm_before
    alpha = norm / (product - ratio * norm / alpha_before)
    direction = residual + ratio * base
    answer = answer + alpha * direction
    residual, image = (
        residual - alpha * (image + ratio * first),
        image - alpha * (again + ratio * second),
    )
    send_sum(2, 0, partial_sums(residual, image))
    send_sum(2, 1, wait_sum(2, 0))
    norm_before, alpha_before = norm, alpha
    norm, product = totals(wait_sum(2, 1))
    ratio = norm / norm_before
    alpha = norm / (product - ratio * norm / alpha_before)
    out[...] = answer + alpha * (residual + ratio * direction)
    for copy in sent:
        copy.wait_send()


def body(mesh_counts, density, base_velocity, cells, offsets, target, stiffness, counts):
    sizes = density.shape
    size_x, size_y, size_z = sizes
    cap = cells.shape[1]
    assert sizes == (8, 8, 128) and min(mesh_counts) > 2
    lanes = 2 * size_z
    number, flat = 27, 9
    turns = ITERS + 1
    near, far = mesh_counts[1] * mesh_counts[2], mesh_counts[0]
    return pl.pallas_call(
        functools.partial(kernel, mesh_counts, sizes),
        out_shape=jax.ShapeDtypeStruct((3, cap), jnp.float32),
        in_specs=[pl.BlockSpec(memory_space=pltpu.HBM)] * 7,
        out_specs=pl.BlockSpec(memory_space=pltpu.VMEM),
        scratch_shapes=[
            pltpu.VMEM((4, size_x, size_y, size_z), jnp.float32),
            pltpu.VMEM((3, cap), jnp.int32),
            pltpu.VMEM((3, cap), jnp.float32),
            pltpu.VMEM((3, cap), jnp.float32),
            pltpu.VMEM((1, cap), jnp.float32),
            pltpu.SMEM((1,), jnp.int32),
            pltpu.VMEM((4, WIDE, TALL, lanes), jnp.float32),
            pltpu.VMEM((4, LOW + HIGH, size_y, size_z), jnp.float32),
            pltpu.VMEM((4, 2, size_y, size_z), jnp.float32),
            pltpu.VMEM((4, 4, size_y, size_z), jnp.float32),
            pltpu.VMEM((4, 4, size_y, size_z), jnp.float32),
            pltpu.VMEM((4, 7, size_y, size_z), jnp.float32),
            pltpu.VMEM((size_y, size_z), jnp.float32),
            pltpu.VMEM((size_y, size_z), jnp.float32),
            pltpu.VMEM((2, flat, size_y, size_z), jnp.float32),
            pltpu.VMEM((number, 3 * (cap // 256), 4, 128), jnp.float32),
            pltpu.VMEM((ITERS, number, 3, cap // 128, 128), jnp.float32),
            pltpu.VMEM((ITERS, near, 2, 128), jnp.float32),
            pltpu.VMEM((ITERS, far, 2, 128), jnp.float32),
            pltpu.VMEM((PATCH_ROWS, cap), jnp.float32),
            pltpu.VMEM((flat, lanes, cap), jnp.bfloat16),
            pltpu.VMEM((flat, lanes, cap), jnp.bfloat16),
            pltpu.VMEM((2, 2 * PATCH_ROWS, cap), jnp.bfloat16),
            pltpu.VMEM((2, flat, 8, cap), jnp.float32),
            pltpu.VMEM((2, WIDE, TALL, size_z), jnp.float32),
            pltpu.VMEM((3, WIDE, TALL, lanes), jnp.float32),
            pltpu.SemaphoreType.DMA((7,)),
            pltpu.SemaphoreType.DMA((turns,)),
            pltpu.SemaphoreType.DMA((turns,)),
            pltpu.SemaphoreType.DMA((ITERS,)),
            pltpu.SemaphoreType.DMA((ITERS,)),
            pltpu.SemaphoreType.DMA((ITERS,)),
            pltpu.SemaphoreType.DMA((ITERS,)),
            pltpu.SemaphoreType.DMA((7,)),
            pltpu.SemaphoreType.DMA((7,)),
        ],
        compiler_params=pltpu.CompilerParams(
            collective_id=0, has_side_effects=True, vmem_limit_bytes=60 * 1024 * 1024
        ),
    )(density, base_velocity, cells, offsets, target, stiffness[None], counts)


def solution(mesh):
    return jax.shard_map(
        functools.partial(body, tuple(mesh.shape[name] for name in AXES)),
        mesh=mesh,
        in_specs=(
            P("gx", "gy", "gz"),
            P(None, "gx", "gy", "gz"),
            P(None, ("gx", "gy", "gz")),
            P(None, ("gx", "gy", "gz")),
            P(None, ("gx", "gy", "gz")),
            P(("gx", "gy", "gz")),
            P(("gx", "gy", "gz")),
        ),
        out_specs=P(None, ("gx", "gy", "gz")),
        check_vma=False,
    )
```

```python
import functools
import itertools

import jax
import jax.numpy as jnp
from jax import lax
from jax.experimental import pallas as pl
from jax.experimental.pallas import tpu as pltpu
from jax.sharding import PartitionSpec as P

ITERS = 3
LOW, HIGH = 2, 3
WIDE, TALL, HALF = 13, 16, 8
STEPS = (0, -1, 1)
MESH_ID = pl.DeviceIdType.MESH
AXES = ("gx", "gy", "gz")


def round_up(value, multiple):
    return -(-value // multiple) * multiple


def span(shift, size):
    return {0: (1, size + 3), -1: (0, 4), 1: (size + 1, 4)}[shift]


def weights(fraction):
    root = jnp.sqrt(1.0 + 4.0 * fraction - 4.0 * fraction * fraction)
    near, far = 3.0 - 2.0 * fraction, 1.0 + 2.0 * fraction
    return ((near - root) / 8.0, (near + root) / 8.0, (far + root) / 8.0, (far - root) / 8.0)


def table(cell, four, shift, size, first, rows):
    place = lax.broadcasted_iota(jnp.int32, (rows, cell.shape[1]), 0).astype(jnp.float32) + first
    apart = place - (cell + (1.0 + shift * size))
    total = jnp.where(apart == 3.0, four[3], 0.0)
    for number in (2, 1, 0):
        total = jnp.where(apart == float(number), four[number], total)
    return total


def split(value):
    high = value.astype(jnp.bfloat16)
    return high, (value - high.astype(jnp.float32)).astype(jnp.bfloat16)


def dot_nt(a, b):
    return lax.dot_general(a, b, (((1,), (1,)), ((), ())), preferred_element_type=jnp.float32)


def dot_nn(a, b):
    return lax.dot_general(a, b, (((1,), (0,)), ((), ())), preferred_element_type=jnp.float32)


def patches():
    found, base = {}, 0
    for step_x, step_y in itertools.product(STEPS, STEPS):
        row, rows = {0: (0, TALL), -1: (0, HALF), 1: (HALF, HALF)}[step_y]
        start, planes = span(step_x, 8)
        if step_x == 0 and step_y:
            planes += 1
        found[step_x, step_y] = (start, planes, row, rows, base)
        base += planes * rows
    return found, base


PATCHES, PATCH_ROWS = patches()
FLAT = list(PATCHES)


def kernel(
    counts, sizes, density, velocity, cells_in, offsets_in, target_in, stiffness_in, count_in, out,
    block, cells_ref, offsets_ref, target_ref, stiffness_ref, count_ref,
    fields, xbuf, ylow, yhigh, below, above, zlow, zhigh, zbuf, nbuf, fbuf, rbuf, sbuf, dbuf,
    txy, thi, tlo, azz, tzz, edge, grid,
    lsem, nsend, nrecv, ssend, srecv, hsend, hrecv,
):
    size_x, size_y, size_z = sizes
    cap = cells_ref.shape[1]
    lanes = fields.shape[3]
    slots = list(itertools.product(STEPS, STEPS, STEPS))
    me = [lax.axis_index(name) for name in AXES]
    sent = []

    def device(offset):
        return tuple(lax.rem(m + (o % n), n) for m, o, n in zip(me, offset, counts))

    def negated(offset):
        return tuple(-o for o in offset)

    near = [o for o in itertools.product([0], range(counts[1]), range(counts[2])) if any(o)]
    far = [(o, 0, 0) for o in range(1, counts[0])]
    whole = [o for o in itertools.product(*[range(n) for n in counts]) if any(o)]
    wrapped = {tuple(o % n for o, n in zip(slot, counts)) for slot in slots if any(slot)}
    peers = sorted(wrapped | set(near) | set(far))
    loads = [
        pltpu.make_async_copy(source, destination, lsem.at[k])
        for k, (source, destination) in enumerate(
            [
                (velocity, block.at[pl.ds(0, 3)]),
                (density, block.at[3]),
                (cells_in, cells_ref),
                (offsets_in, offsets_ref),
                (target_in, target_ref),
                (stiffness_in, stiffness_ref),
                (count_in, count_ref),
            ]
        )
    ]
    for load in loads:
        load.start()
    barrier = pltpu.get_barrier_semaphore()
    for peer in peers:
        pl.semaphore_signal(barrier, inc=1, device_id=device(peer), device_id_type=MESH_ID)

    def go(copies):
        for copy in copies:
            copy.start()

    def every(ref, send, receive):
        copy = pltpu.make_async_remote_copy(
            src_ref=ref,
            dst_ref=ref,
            send_sem=send,
            recv_sem=receive,
            device_id=device(far[0]),
            device_id_type=MESH_ID,
        )
        sent.append(copy)
        return copy

    def neighbour_copy(turn, number):
        return pltpu.make_async_remote_copy(
            src_ref=fbuf.at[turn - 1, 0] if turn else nbuf.at[0],
            dst_ref=fbuf.at[turn - 1, number] if turn else nbuf.at[number],
            send_sem=nsend.at[turn],
            recv_sem=nrecv.at[turn],
            device_id=device(negated(slots[number])),
            device_id_type=MESH_ID,
        )

    def send_round(turn):
        far_first = sorted(range(1, len(slots)), key=lambda k: (-sum(map(abs, slots[k])), k))
        go([neighbour_copy(turn, number) for number in far_first])

    def wait_round(turn):
        others = pl.ds(1, len(slots) - 1)
        landed = fbuf.at[turn - 1, others] if turn else nbuf.at[others]
        every(landed, nsend.at[turn], nrecv.at[turn]).wait_recv()

    def away(offset):
        return sum(min(o, n - o) for o, n in zip(offset, counts))

    stages = {
        "near": (near, rbuf.at[0], ssend.at[0], srecv.at[0]),
        "far": (far, sbuf.at[0], ssend.at[1], srecv.at[1]),
        1: (whole, dbuf.at[0], ssend.at[2], srecv.at[2]),
        2: (whole, dbuf.at[1], ssend.at[3], srecv.at[3]),
    }

    def send_sum(stage, value):
        members, buffer, send, receive = stages[stage]
        buffer[0] = value
        for number in sorted(range(len(members)), key=lambda k: (-away(members[k]), k)):
            pltpu.make_async_remote_copy(
                src_ref=buffer.at[0],
                dst_ref=buffer.at[number + 1],
                send_sem=send,
                recv_sem=receive,
                device_id=device(negated(members[number])),
                device_id_type=MESH_ID,
            ).start()

    def wait_sum(stage):
        members, buffer, send, receive = stages[stage]
        every(buffer.at[pl.ds(1, len(members))], send, receive).wait_recv()
        total = buffer[...]
        while total.shape[0] > 1:
            half = total.shape[0] // 2
            total = total[:half] + total[half:]
        return total[0]

    def put(turn, vector):
        for c in range(3):
            for part in range(cap // 128):
                fbuf[turn - 1, 0, c, pl.ds(part, 1), :] = vector[
                    c : c + 1, part * 128 : part * 128 + 128
                ]

    def joined(ref, at, number, k):
        return jnp.concatenate(
            [ref[at, number, k, pl.ds(part, 1), :] for part in range(cap // 128)], axis=1
        )

    def mark(number, k):
        each = cap // 128
        parts = [divmod(k * each + part, 4) for part in range(each)]
        return jnp.concatenate([nbuf[number, a, pl.ds(b, 1), :] for a, b in parts], axis=1)

    def halo_copy(number, source, target, step):
        return pltpu.make_async_remote_copy(
            src_ref=source,
            dst_ref=target,
            send_sem=hsend.at[number],
            recv_sem=hrecv.at[number],
            device_id=device(negated(step)),
            device_id_type=MESH_ID,
        )

    flows, scalars, edges = [], [], []
    plane_of = {-1: (size_x - LOW, LOW, 0), 1: (0, HIGH, LOW)}
    low_of = {-1: (1, 1, 0), 0: (0, 2, 1), 1: (0, 1, 3)}
    high_of = {-1: (3, 1, 0), 0: (0, 4, 1), 1: (0, 2, 5)}
    spaces = ((block, xbuf, plane_of), (ylow, below, low_of), (yhigh, above, high_of))
    corners_first = sorted(FLAT, key=lambda o: -abs(o[0]) - abs(o[1]))
    halves = (pl.ds(0, 3), pl.ds(3, 1))
    for kind, copies in enumerate((flows, scalars)):
        for step_x, step_y in corners_first:
            if step_x == step_y == 0:
                continue
            space = 0 if step_y == 0 else 1 if step_y < 0 else 2
            source, target, where = spaces[space]
            first, many, at = where[step_x]
            copies.append(
                halo_copy(
                    3 * kind + space,
                    source.at[halves[kind], pl.ds(first, many)],
                    target.at[halves[kind], pl.ds(at, many)],
                    (step_x, step_y, 0),
                )
            )
    for step_x, step_y in corners_first:
        for side, step_z in enumerate((-1, 1)):
            edges.append(
                halo_copy(
                    6,
                    (zlow, zhigh)[side],
                    zbuf.at[side, FLAT.index((step_x, step_y))],
                    (step_x, step_y, step_z),
                )
            )

    def wait_halos(kind):
        for space, (_, target, _) in enumerate(spaces):
            at = 3 * kind + space
            every(target.at[halves[kind]], hsend.at[at], hrecv.at[at]).wait_recv()
        if kind == 0:
            every(zbuf, hsend.at[6], hrecv.at[6]).wait_recv()

    lane = lax.broadcasted_iota(jnp.int32, (size_y, size_z), 1)
    row = lax.broadcasted_iota(jnp.int32, (size_y, size_z), 0)

    def turned(value, by, axis):
        by %= value.shape[axis]
        return pltpu.roll(value, by, axis) if by else value

    def pack():
        low = [jnp.zeros((size_y, size_z), jnp.float32)] * 2
        high = [jnp.zeros((size_y, size_z), jnp.float32)] * 2
        for c in range(4):
            tiles_low = [None] * 2
            tiles_high = [None] * 4
            for plane in range(size_x):
                own = block[c, plane]
                t, q = divmod(plane, 4)
                moved = turned(own, 2 * q - 6, 0)
                tiles_low[t] = moved if q == 0 else jnp.where(row // 2 == q, moved, tiles_low[t])
                t, q = divmod(plane, 2)
                moved = turned(own, 4 * q, 0)
                tiles_high[t] = moved if q == 0 else jnp.where(row // 4 == q, moved, tiles_high[t])
                at = c * size_x + plane
                chain = plane % 2
                low[chain] = jnp.where(
                    lane // 2 == at, turned(own, 2 * at - (size_z - LOW), 1), low[chain]
                )
                high[chain] = jnp.where(lane // 4 == at, turned(own, 4 * at, 1), high[chain])
            for t in range(2):
                ylow[c, t] = tiles_low[t]
            for t in range(4):
                yhigh[c, t] = tiles_high[t]
        zlow[...] = jnp.where(lane // 2 % 2 == 0, low[0], low[1])
        zhigh[...] = jnp.where(lane // 4 % 2 == 0, high[0], high[1])

    def tall_of(down, own, up):
        moved = turned(own, LOW, 0)
        return (
            jnp.where(row < LOW, down, moved),
            jnp.where(row < LOW, moved, up),
        )

    def widen(components, first):
        sides = {}
        for step_x in STEPS:
            for side in range(2):
                down, own, up = (zbuf[side, FLAT.index((step_x, step_y))] for step_y in (-1, 0, 1))
                sides[step_x, side] = tall_of(turned(down, LOW, 0), own, turned(up, LOW, 0))
        for plane in range(WIDE):
            if plane < LOW:
                step_x, x = -1, plane + size_x - LOW
            elif plane < LOW + size_x:
                step_x, x = 0, plane - LOW
            else:
                step_x, x = 1, plane - LOW - size_x
            for c in components:
                own = block[c, x] if step_x == 0 else xbuf[c, plane if step_x < 0 else plane - size_x]
                source, _, at = low_of[step_x]
                down = turned(below[c, at + x // 4 - source], -2 * (x % 4), 0)
                source, _, at = high_of[step_x]
                up = turned(above[c, at + x // 2 - source], LOW - 4 * (x % 2), 0)
                talls = tall_of(down, own, up)
                index = c * size_x + x
                for half in range(2):
                    moved = turned(talls[half], LOW, 1)
                    start = turned(sides[step_x, 0][half], -2 * index, 1)
                    end = turned(sides[step_x, 1][half], LOW - 4 * index, 1)
                    left = jnp.where(lane < LOW, start, moved)
                    right = jnp.where(lane < LOW, moved, jnp.where(lane < LOW + HIGH, end, first))
                    if half:
                        left = jnp.where(row < LOW + HIGH, left, first)
                        right = jnp.where(row < LOW + HIGH, right, first)
                    if c == 3:
                        left, right = lax.rsqrt(left), lax.rsqrt(right)
                    rows = pl.ds(half * size_y, size_y)
                    fields[c, plane, rows, pl.ds(0, size_z)] = left
                    fields[c, plane, rows, pl.ds(size_z, size_z)] = right

    def tables(step_x, step_y, step_z):
        number = slots.index((step_x, step_y, step_z))
        cells = [mark(number, k) for k in range(3)]
        fours = [weights(mark(number, k + 3)) for k in range(3)]
        start, planes, first_row, rows, base = PATCHES[step_x, step_y]
        first = start // 8 * 8
        tall = round_up(start + planes - first, 8)
        tab_x = table(cells[0], fours[0], step_x, size_x, float(first), tall)
        tab_y = table(cells[1], fours[1], step_y, size_y, float(first_row), rows)
        return cells[2], fours[2], [
            tab_x[start - first + plane : start - first + plane + 1] * tab_y for plane in range(planes)
        ]

    def build_main(step_x, step_y):
        cell, four, products = tables(step_x, step_y, 0)
        start, planes, first_row, rows, base = PATCHES[step_x, step_y]
        for plane, product in enumerate(products):
            txy[pl.ds(base + plane * rows, rows), :] = product
        k = FLAT.index((step_x, step_y))
        used = round_up(size_z + 5, 16)
        high, low = split(table(cell, four, 0, size_z, 0.0, used))
        for ref, part in ((thi, high), (tlo, low)):
            ref[k, pl.ds(0, used), :] = part
            ref[k, pl.ds(used, lanes - used), :] = jnp.zeros((lanes - used, cap), jnp.bfloat16)

    def build_side(step_x, step_y, side):
        cell, four, products = tables(step_x, step_y, (-1, 1)[side])
        start, planes, first_row, rows, base = PATCHES[step_x, step_y]
        many = planes * rows
        high, low = split(jnp.concatenate(products, axis=0))
        azz[side, pl.ds(2 * base, many), :] = high
        azz[side, pl.ds(2 * base + many, many), :] = low
        k = FLAT.index((step_x, step_y))
        tzz[side, k] = table(cell, four, (-1, 1)[side], size_z, float(side * size_z), 8)

    _, own_planes, _, _, _ = PATCHES[0, 0]
    own_rows = own_planes * TALL

    def interpolate(field):
        high, low = split(field.reshape(3 * own_rows, lanes))
        z_high, z_low = thi[0], tlo[0]
        part = dot_nn(high, z_high) + dot_nn(low, z_high) + dot_nn(high, z_low)
        plane = txy[pl.ds(0, own_rows), :]
        return jnp.concatenate(
            [
                jnp.sum(part[c * own_rows : (c + 1) * own_rows] * plane, axis=0, keepdims=True)
                for c in range(3)
            ],
            axis=0,
        )

    def spread_main(turn, step_x, step_y):
        start, planes, first_row, rows, base = PATCHES[step_x, step_y]
        number = slots.index((step_x, step_y, 0))
        k = FLAT.index((step_x, step_y))
        plane = txy[pl.ds(base, planes * rows), :]
        high, low = split(
            jnp.concatenate([plane * joined(fbuf, turn - 1, number, c) for c in range(3)], axis=0)
        )
        part = dot_nt(high, thi[k]) + dot_nt(low, thi[k]) + dot_nt(high, tlo[k])
        part = part.reshape(3, planes, rows, lanes)
        if number == 0:
            for edge_plane in (0, WIDE - 1):
                grid[:, edge_plane] = jnp.zeros((3, TALL, lanes), jnp.float32)
            grid[:, pl.ds(start, planes)] = part
        else:
            grid[:, pl.ds(start, planes), pl.ds(first_row, rows)] += part

    def spread_side(turn, step_x, step_y, side):
        start, planes, first_row, rows, base = PATCHES[step_x, step_y]
        number = slots.index((step_x, step_y, (-1, 1)[side]))
        k = FLAT.index((step_x, step_y))
        many = planes * rows
        tab = tzz[side, k]
        pieces = [tab * joined(fbuf, turn - 1, number, c) for c in range(3)]
        high, low = split(jnp.concatenate(pieces + [jnp.zeros_like(tab)], axis=0))
        part = dot_nt(
            azz[side, pl.ds(2 * base, 2 * many), :], jnp.concatenate([high, low], axis=0)
        )
        part = (part[:many] + part[many:]).reshape(planes, rows, 64)
        where = (side, pl.ds(start, planes), pl.ds(first_row, rows), pl.ds(0, 64))
        if (step_x, step_y) == (0, 0):
            edge[where] = part
        else:
            edge[where] += part

    def finish_sides():
        inside = lax.broadcasted_iota(jnp.int32, (WIDE, TALL, size_z), 2) < 8
        for side in range(2):
            both = edge[side]
            both = both + turned(both, -32, 2)
            for c in range(3):
                part = jnp.where(inside, turned(both, -8 * c, 2), 0.0)
                grid[c, :, :, pl.ds(side * size_z, size_z)] += part

    def spread_rest(turn):
        wait_round(turn)
        for side in range(2):
            for edge_plane in (0, WIDE - 1):
                edge[side, edge_plane] = jnp.zeros((TALL, size_z), jnp.float32)
        for step_x, step_y in FLAT:
            if step_x or step_y:
                spread_main(turn, step_x, step_y)
        for side in range(2):
            for step_x, step_y in FLAT:
                spread_side(turn, step_x, step_y, side)
        finish_sides()

    def add(value, axis):
        return turned(value, -1, axis) + turned(value, 1, axis)

    def sub(value, axis):
        return turned(value, -1, axis) - turned(value, 1, axis)

    def respond():
        scale = fields[3]
        mx, my, mz = (scale * grid[c] for c in range(3))
        slope_y, slope_z = sub(my, 1), sub(mz, 2)
        sum_x = 2.0 * mx + add(mx, 1) + add(mx, 2)
        slope = slope_y + slope_z
        px = sum_x[2:] + sum_x[:-2] + slope[2:] - slope[:-2]
        slope_x = mx[2:] - mx[:-2]
        sum_y = (2.0 * my + add(my, 2))[1:-1] + my[2:] + my[:-2]
        py = add(sum_y, 1) + sub(slope_x + slope_z[1:-1], 1)
        sum_z = (2.0 * mz + add(mz, 1))[1:-1] + mz[2:] + mz[:-2]
        pz = add(sum_z, 2) + sub(slope_x + slope_y[1:-1], 2)
        half = scale[1:-1] * 0.5
        return jnp.stack(
            [half * (m[1:-1] + p * (1.0 / 12.0)) for m, p in ((mx, px), (my, py), (mz, pz))]
        )

    def apply(turn, vector):
        spread_rest(turn)
        return live * (interpolate(respond()) + stiffness * vector)

    left_half = lax.broadcasted_iota(jnp.int32, (1, 128), 1) < 64

    def partial_sums(residual, image):
        folded = []
        for other in (residual, image):
            line = jnp.sum(residual * other, axis=0, keepdims=True)
            total = line[:, :128]
            for at in range(128, cap, 128):
                total = total + line[:, at : at + 128]
            folded.append(total + turned(total, 64, 1))
        return jnp.where(left_half, folded[0], folded[1])

    def totals(tile):
        return (
            jnp.sum(jnp.where(left_half, tile, 0.0), axis=1, keepdims=True),
            jnp.sum(jnp.where(left_half, 0.0, tile), axis=1, keepdims=True),
        )

    loads[0].wait()
    loads[1].wait()
    pack()
    loads[2].wait()
    loads[3].wait()
    each = cap // 128
    for k, size in enumerate(sizes):
        local = (cells_ref[pl.ds(k, 1), :] - me[k] * size).astype(jnp.float32)
        for values, at in ((local, k), (offsets_ref[pl.ds(k, 1), :], k + 3)):
            for part in range(each):
                a, b = divmod(at * each + part, 4)
                nbuf[0, a, pl.ds(b, 1), :] = values[:, part * 128 : part * 128 + 128]
    for load in loads[4:]:
        load.wait()
    pl.semaphore_wait(barrier, len(peers))
    go(flows)
    go(edges)
    send_round(0)
    go(scalars)
    target, stiffness = target_ref[...], stiffness_ref[...]
    live = (lax.broadcasted_iota(jnp.int32, (1, cap), 1) < count_ref[0]).astype(jnp.float32)
    build_main(0, 0)
    edge[...] = jnp.zeros_like(edge)
    wait_halos(0)
    widen((0, 1, 2), 0.0)
    base = live * (target - interpolate(fields[pl.ds(0, 3), pl.ds(1, own_planes)]))
    put(1, base)
    send_round(1)
    spread_main(1, 0, 0)
    wait_round(0)
    for step_x, step_y in FLAT:
        if step_x or step_y:
            build_main(step_x, step_y)
        build_side(step_x, step_y, 0)
        build_side(step_x, step_y, 1)
    wait_halos(1)
    widen((3,), 1.0)
    first = apply(1, base)
    send_sum("near", partial_sums(base, first))
    put(2, first)
    send_round(2)
    spread_main(2, 0, 0)
    send_sum("far", wait_sum("near"))
    second = apply(2, first)
    put(3, second)
    send_round(3)
    spread_main(3, 0, 0)
    norm, product = totals(wait_sum("far"))
    alpha = norm / product
    answer = alpha * base
    residual, image = base - alpha * first, first - alpha * second
    send_sum(1, partial_sums(residual, image))
    third = apply(3, second)
    again = second - alpha * third
    norm_before, alpha_before = norm, alpha
    norm, product = totals(wait_sum(1))
    ratio = norm / norm_before
    alpha = norm / (product - ratio * norm / alpha_before)
    direction = residual + ratio * base
    answer = answer + alpha * direction
    residual, image = (
        residual - alpha * (image + ratio * first),
        image - alpha * (again + ratio * second),
    )
    send_sum(2, partial_sums(residual, image))
    norm_before, alpha_before = norm, alpha
    norm, product = totals(wait_sum(2))
    ratio = norm / norm_before
    alpha = norm / (product - ratio * norm / alpha_before)
    out[...] = answer + alpha * (residual + ratio * direction)
    for copy in sent:
        copy.wait_send()


def body(mesh_counts, density, base_velocity, cells, offsets, target, stiffness, counts):
    sizes = density.shape
    size_x, size_y, size_z = sizes
    cap = cells.shape[1]
    assert sizes == (8, 8, 128) and min(mesh_counts) > 2
    lanes = 2 * size_z
    number, flat = 27, 9
    turns = ITERS + 1
    near, far = mesh_counts[1] * mesh_counts[2], mesh_counts[0]
    return pl.pallas_call(
        functools.partial(kernel, mesh_counts, sizes),
        out_shape=jax.ShapeDtypeStruct((3, cap), jnp.float32),
        in_specs=[pl.BlockSpec(memory_space=pltpu.HBM)] * 7,
        out_specs=pl.BlockSpec(memory_space=pltpu.VMEM),
        scratch_shapes=[
            pltpu.VMEM((4, size_x, size_y, size_z), jnp.float32),
            pltpu.VMEM((3, cap), jnp.int32),
            pltpu.VMEM((3, cap), jnp.float32),
            pltpu.VMEM((3, cap), jnp.float32),
            pltpu.VMEM((1, cap), jnp.float32),
            pltpu.SMEM((1,), jnp.int32),
            pltpu.VMEM((4, WIDE, TALL, lanes), jnp.float32),
            pltpu.VMEM((4, LOW + HIGH, size_y, size_z), jnp.float32),
            pltpu.VMEM((4, 2, size_y, size_z), jnp.float32),
            pltpu.VMEM((4, 4, size_y, size_z), jnp.float32),
            pltpu.VMEM((4, 4, size_y, size_z), jnp.float32),
            pltpu.VMEM((4, 7, size_y, size_z), jnp.float32),
            pltpu.VMEM((size_y, size_z), jnp.float32),
            pltpu.VMEM((size_y, size_z), jnp.float32),
            pltpu.VMEM((2, flat, size_y, size_z), jnp.float32),
            pltpu.VMEM((number, 3 * (cap // 256), 4, 128), jnp.float32),
            pltpu.VMEM((ITERS, number, 3, cap // 128, 128), jnp.float32),
            pltpu.VMEM((1, near, 1, 128), jnp.float32),
            pltpu.VMEM((1, far, 1, 128), jnp.float32),
            pltpu.VMEM((2, near * far, 1, 128), jnp.float32),
            pltpu.VMEM((PATCH_ROWS, cap), jnp.float32),
            pltpu.VMEM((flat, lanes, cap), jnp.bfloat16),
            pltpu.VMEM((flat, lanes, cap), jnp.bfloat16),
            pltpu.VMEM((2, 2 * PATCH_ROWS, cap), jnp.bfloat16),
            pltpu.VMEM((2, flat, 8, cap), jnp.float32),
            pltpu.VMEM((2, WIDE, TALL, size_z), jnp.float32),
            pltpu.VMEM((3, WIDE, TALL, lanes), jnp.float32),
            pltpu.SemaphoreType.DMA((7,)),
            pltpu.SemaphoreType.DMA((turns,)),
            pltpu.SemaphoreType.DMA((turns,)),
            pltpu.SemaphoreType.DMA((4,)),
            pltpu.SemaphoreType.DMA((4,)),
            pltpu.SemaphoreType.DMA((7,)),
            pltpu.SemaphoreType.DMA((7,)),
        ],
        compiler_params=pltpu.CompilerParams(
            collective_id=0, has_side_effects=True, vmem_limit_bytes=60 * 1024 * 1024
        ),
    )(density, base_velocity, cells, offsets, target, stiffness[None], counts)


def solution(mesh):
    return jax.shard_map(
        functools.partial(body, tuple(mesh.shape[name] for name in AXES)),
        mesh=mesh,
        in_specs=(
            P("gx", "gy", "gz"),
            P(None, "gx", "gy", "gz"),
            P(None, ("gx", "gy", "gz")),
            P(None, ("gx", "gy", "gz")),
            P(None, ("gx", "gy", "gz")),
            P(("gx", "gy", "gz")),
            P(("gx", "gy", "gz")),
        ),
        out_specs=P(None, ("gx", "gy", "gz")),
        check_vma=False,
    )
```

```python
import functools
import itertools

import jax
import jax.numpy as jnp
from jax import lax
from jax.experimental import pallas as pl
from jax.experimental.pallas import tpu as pltpu
from jax.sharding import PartitionSpec as P

ITERS = 3
LOW = 2
KINDS = (((0, 1, 2), 1, 2, 2), ((3,), 2, 3, 4))
WIDE, TALL, HALF = 13, 16, 8
STEPS = (0, -1, 1)
MESH_ID = pl.DeviceIdType.MESH
AXES = ("gx", "gy", "gz")


def round_up(value, multiple):
    return -(-value // multiple) * multiple


def span(shift, size):
    return {0: (1, size + 3), -1: (0, 4), 1: (size + 1, 4)}[shift]


def weights(fraction):
    root = jnp.sqrt(1.0 + 4.0 * fraction - 4.0 * fraction * fraction)
    near, far = 3.0 - 2.0 * fraction, 1.0 + 2.0 * fraction
    return ((near - root) / 8.0, (near + root) / 8.0, (far + root) / 8.0, (far - root) / 8.0)


def table(cell, four, shift, size, first, rows):
    place = lax.broadcasted_iota(jnp.int32, (rows, cell.shape[1]), 0).astype(jnp.float32) + first
    apart = place - (cell + (1.0 + shift * size))
    total = jnp.where(apart == 3.0, four[3], 0.0)
    for number in (2, 1, 0):
        total = jnp.where(apart == float(number), four[number], total)
    return total


def split(value):
    high = value.astype(jnp.bfloat16)
    return high, (value - high.astype(jnp.float32)).astype(jnp.bfloat16)


def dot_nt(a, b):
    return lax.dot_general(a, b, (((1,), (1,)), ((), ())), preferred_element_type=jnp.float32)


def dot_nn(a, b):
    return lax.dot_general(a, b, (((1,), (0,)), ((), ())), preferred_element_type=jnp.float32)


def patches():
    found, base = {}, 0
    for step_x, step_y in itertools.product(STEPS, STEPS):
        row, rows = {0: (0, TALL), -1: (0, HALF), 1: (HALF, HALF)}[step_y]
        start, planes = span(step_x, 8)
        if step_x == 0 and step_y:
            planes += 1
        found[step_x, step_y] = (start, planes, row, rows, base)
        base += planes * rows
    return found, base


PATCHES, PATCH_ROWS = patches()
FLAT = list(PATCHES)


def kernel(
    counts, sizes, density, velocity, cells_in, offsets_in, target_in, stiffness_in, count_in, out,
    block, cells_ref, offsets_ref, target_ref, stiffness_ref, count_ref,
    fields, low_v, high_v, start_v, end_v, x_v, below_v, above_v, z_v,
    low_d, high_d, start_d, end_d, x_d, below_d, above_d, z_d, nbuf, fbuf, rbuf, sbuf, dbuf,
    txy, thi, tlo, azz, tzz, edge, grid,
    lsem, nsend, nrecv, ssend, srecv, hsend, hrecv,
):
    size_x, size_y, size_z = sizes
    cap = cells_ref.shape[1]
    lanes = fields.shape[3]
    slots = list(itertools.product(STEPS, STEPS, STEPS))
    me = [lax.axis_index(name) for name in AXES]
    sent = []
    packs = ((low_v, high_v, start_v, end_v), (low_d, high_d, start_d, end_d))
    landing = ((x_v, below_v, above_v, z_v), (x_d, below_d, above_d, z_d))

    def device(offset):
        return tuple(lax.rem(m + (o % n), n) for m, o, n in zip(me, offset, counts))

    def negated(offset):
        return tuple(-o for o in offset)

    near = [o for o in itertools.product([0], range(counts[1]), range(counts[2])) if any(o)]
    far = [(o, 0, 0) for o in range(1, counts[0])]
    whole = [o for o in itertools.product(*[range(n) for n in counts]) if any(o)]
    wrapped = {tuple(o % n for o, n in zip(slot, counts)) for slot in slots if any(slot)}
    half_way = {(counts[0] // 2, 0, 0), (0, counts[1] // 2, 0)}
    peers = sorted(wrapped | half_way)
    loads = [
        pltpu.make_async_copy(source, destination, lsem.at[k])
        for k, (source, destination) in enumerate(
            [
                (velocity, block.at[pl.ds(0, 3)]),
                (density, block.at[3]),
                (cells_in, cells_ref),
                (offsets_in, offsets_ref),
                (target_in, target_ref),
                (stiffness_in, stiffness_ref),
                (count_in, count_ref),
            ]
        )
    ]
    barrier = pltpu.get_barrier_semaphore()
    for peer in peers:
        pl.semaphore_signal(barrier, inc=1, device_id=device(peer), device_id_type=MESH_ID)
    for load in loads:
        load.start()

    def go(copies):
        for copy in copies:
            copy.start()

    def every(ref, send, receive):
        copy = pltpu.make_async_remote_copy(
            src_ref=ref,
            dst_ref=ref,
            send_sem=send,
            recv_sem=receive,
            device_id=device(far[0]),
            device_id_type=MESH_ID,
        )
        sent.append(copy)
        return copy

    def neighbour_copy(turn, number):
        return pltpu.make_async_remote_copy(
            src_ref=fbuf.at[turn - 1, 0] if turn else nbuf.at[0],
            dst_ref=fbuf.at[turn - 1, number] if turn else nbuf.at[number],
            send_sem=nsend.at[turn],
            recv_sem=nrecv.at[turn],
            device_id=device(negated(slots[number])),
            device_id_type=MESH_ID,
        )

    def send_round(turn):
        far_first = sorted(range(1, len(slots)), key=lambda k: (-sum(map(abs, slots[k])), k))
        go([neighbour_copy(turn, number) for number in far_first])

    def wait_round(turn):
        others = pl.ds(1, len(slots) - 1)
        landed = fbuf.at[turn - 1, others] if turn else nbuf.at[others]
        every(landed, nsend.at[turn], nrecv.at[turn]).wait_recv()

    def away(offset):
        return sum(min(o, n - o) for o, n in zip(offset, counts))

    stages = {
        "near": (near, rbuf.at[0], ssend.at[0], srecv.at[0]),
        "far": (far, sbuf.at[0], ssend.at[1], srecv.at[1]),
        1: (whole, dbuf.at[0], ssend.at[2], srecv.at[2]),
        2: (whole, dbuf.at[1], ssend.at[3], srecv.at[3]),
    }

    def send_sum(stage, value):
        members, buffer, send, receive = stages[stage]
        buffer[0] = value
        for number in sorted(range(len(members)), key=lambda k: (-away(members[k]), k)):
            pltpu.make_async_remote_copy(
                src_ref=buffer.at[0],
                dst_ref=buffer.at[number + 1],
                send_sem=send,
                recv_sem=receive,
                device_id=device(negated(members[number])),
                device_id_type=MESH_ID,
            ).start()

    def wait_sum(stage):
        members, buffer, send, receive = stages[stage]
        every(buffer.at[pl.ds(1, len(members))], send, receive).wait_recv()
        total = buffer[...]
        while total.shape[0] > 1:
            half = total.shape[0] // 2
            total = total[:half] + total[half:]
        return total[0]

    def put(turn, vector):
        for c in range(3):
            for part in range(cap // 128):
                fbuf[turn - 1, 0, c, pl.ds(part, 1), :] = vector[
                    c : c + 1, part * 128 : part * 128 + 128
                ]

    def joined(ref, at, number, k):
        return jnp.concatenate(
            [ref[at, number, k, pl.ds(part, 1), :] for part in range(cap // 128)], axis=1
        )

    def mark(number, k):
        each = cap // 128
        parts = [divmod(k * each + part, 4) for part in range(each)]
        return jnp.concatenate([nbuf[number, a, pl.ds(b, 1), :] for a, b in parts], axis=1)

    def halo_copy(number, source, target, step):
        return pltpu.make_async_remote_copy(
            src_ref=source,
            dst_ref=target,
            send_sem=hsend.at[number],
            recv_sem=hrecv.at[number],
            device_id=device(negated(step)),
            device_id_type=MESH_ID,
        )

    corners_first = sorted(FLAT, key=lambda o: -abs(o[0]) - abs(o[1]))

    def halos(kind):
        parts, low, high, slot = KINDS[kind]
        (source_x, source_low, source_high, source_start, source_end), targets = (
            (block.at[pl.ds(parts[0], len(parts))], *packs[kind]),
            landing[kind],
        )
        more = -(-high * slot // size_y)
        spaces = (
            (source_x, targets[0], {-1: (size_x - low, low, 0), 1: (0, high, low)}),
            (source_low, targets[1], {-1: (low - 1, 1, 0), 0: (0, low, 1), 1: (0, 1, low + 1)}),
            (source_high, targets[2], {-1: (slot - 1, 1, 0), 0: (0, slot, 1), 1: (0, more, slot + 1)}),
        )
        copies = []
        for step_x, step_y in corners_first:
            if step_x or step_y:
                space = 0 if step_y == 0 else 1 if step_y < 0 else 2
                source, target, where = spaces[space]
                first, many, at = where[step_x]
                copies.append(
                    halo_copy(
                        4 * kind + space,
                        source.at[:, pl.ds(first, many)],
                        target.at[:, pl.ds(at, many)],
                        (step_x, step_y, 0),
                    )
                )
        for step_x, step_y in corners_first:
            for side, step_z in enumerate((-1, 1)):
                copies.append(
                    halo_copy(
                        4 * kind + 3,
                        (source_start, source_end)[side],
                        targets[3].at[side, FLAT.index((step_x, step_y))],
                        (step_x, step_y, step_z),
                    )
                )
        return copies

    def wait_halos(kind):
        for space, target in enumerate(landing[kind]):
            at = 4 * kind + space
            every(target, hsend.at[at], hrecv.at[at]).wait_recv()

    lane = lax.broadcasted_iota(jnp.int32, (size_y, size_z), 1)
    row = lax.broadcasted_iota(jnp.int32, (size_y, size_z), 0)

    def turned(value, by, axis):
        by %= value.shape[axis]
        return pltpu.roll(value, by, axis) if by else value

    def pack(kind):
        parts, low, high, slot = KINDS[kind]
        source_low, source_high, source_start, source_end = packs[kind]
        starts = [jnp.zeros((size_y, size_z), jnp.float32)] * 2
        ends = [jnp.zeros((size_y, size_z), jnp.float32)] * 2
        for i, c in enumerate(parts):
            tiles_low, tiles_high = [None] * low, [None] * slot
            for plane in range(size_x):
                own = block[c, plane]
                t, q = divmod(plane, size_y // low)
                moved = turned(own, low * (q + 1) - size_y, 0)
                tiles_low[t] = moved if q == 0 else jnp.where(row // low == q, moved, tiles_low[t])
                t, q = divmod(plane, size_y // slot)
                moved = turned(own, slot * q, 0)
                tiles_high[t] = moved if q == 0 else jnp.where(row // slot == q, moved, tiles_high[t])
                at = i * size_x + plane
                chain = plane % 2
                starts[chain] = jnp.where(
                    lane // low == at, turned(own, low * (at + 1) - size_z, 1), starts[chain]
                )
                ends[chain] = jnp.where(lane // slot == at, turned(own, slot * at, 1), ends[chain])
            for t in range(low):
                source_low[i, t] = tiles_low[t]
            for t in range(slot):
                source_high[i, t] = tiles_high[t]
        source_start[...] = jnp.where(lane // low % 2 == 0, starts[0], starts[1])
        source_end[...] = jnp.where(lane // slot % 2 == 0, ends[0], ends[1])

    def tall_of(down, own, up):
        moved = turned(own, LOW, 0)
        return jnp.where(row < LOW, down, moved), jnp.where(row < LOW, moved, up)

    def widen(kind):
        parts, low, high, slot = KINDS[kind]
        xbuf, below, above, zbuf = landing[kind]
        blank = 1.0 if kind else 0.0
        sides = {}
        for step_x in STEPS:
            for side in range(2):
                down, own, up = (zbuf[side, FLAT.index((step_x, step_y))] for step_y in (-1, 0, 1))
                sides[step_x, side] = tall_of(turned(down, LOW, 0), own, turned(up, LOW, 0))
        for x in range(-low, size_x + high):
            step_x = -1 if x < 0 else 0 if x < size_x else 1
            inner = x - step_x * size_x
            for i, c in enumerate(parts):
                own = block[c, x] if step_x == 0 else xbuf[i, x + low if step_x < 0 else x - size_x + low]
                t, q = divmod(inner, size_y // low)
                t = (0, t + 1, low + 1)[step_x + 1]
                down = turned(below[i, t], LOW - low * (q + 1), 0)
                t, q = divmod(inner, size_y // slot)
                t = (0, t + 1, t + slot + 1)[step_x + 1]
                up = turned(above[i, t], LOW - slot * q, 0)
                if low < LOW:
                    down = jnp.where(row >= LOW - low, down, blank)
                talls = tall_of(down, own, jnp.where(row < LOW + high, up, blank))
                at = i * size_x + inner
                for half in range(2):
                    moved = turned(talls[half], LOW, 1)
                    start = turned(sides[step_x, 0][half], LOW - low * (at + 1), 1)
                    end = turned(sides[step_x, 1][half], LOW - slot * at, 1)
                    if low < LOW:
                        start = jnp.where(lane >= LOW - low, start, blank)
                    left = jnp.where(lane < LOW, start, moved)
                    right = jnp.where(lane < LOW, moved, jnp.where(lane < LOW + high, end, blank))
                    if half:
                        left = jnp.where(row < LOW + high, left, blank)
                        right = jnp.where(row < LOW + high, right, blank)
                    if kind:
                        left, right = lax.rsqrt(left), lax.rsqrt(right)
                    rows = pl.ds(half * size_y, size_y)
                    fields[c, x + LOW, rows, pl.ds(0, size_z)] = left
                    fields[c, x + LOW, rows, pl.ds(size_z, size_z)] = right

    def tables(step_x, step_y, step_z):
        number = slots.index((step_x, step_y, step_z))
        cells = [mark(number, k) for k in range(3)]
        fours = [weights(mark(number, k + 3)) for k in range(3)]
        start, planes, first_row, rows, base = PATCHES[step_x, step_y]
        first = start // 8 * 8
        tall = round_up(start + planes - first, 8)
        tab_x = table(cells[0], fours[0], step_x, size_x, float(first), tall)
        tab_y = table(cells[1], fours[1], step_y, size_y, float(first_row), rows)
        return cells[2], fours[2], [
            tab_x[start - first + plane : start - first + plane + 1] * tab_y for plane in range(planes)
        ]

    def build_main(step_x, step_y):
        cell, four, products = tables(step_x, step_y, 0)
        start, planes, first_row, rows, base = PATCHES[step_x, step_y]
        for plane, product in enumerate(products):
            txy[pl.ds(base + plane * rows, rows), :] = product
        k = FLAT.index((step_x, step_y))
        used = round_up(size_z + 5, 16)
        high, low = split(table(cell, four, 0, size_z, 0.0, used))
        for ref, part in ((thi, high), (tlo, low)):
            ref[k, pl.ds(0, used), :] = part
            ref[k, pl.ds(used, lanes - used), :] = jnp.zeros((lanes - used, cap), jnp.bfloat16)

    def build_side(step_x, step_y, side):
        cell, four, products = tables(step_x, step_y, (-1, 1)[side])
        start, planes, first_row, rows, base = PATCHES[step_x, step_y]
        many = planes * rows
        high, low = split(jnp.concatenate(products, axis=0))
        azz[side, pl.ds(2 * base, many), :] = high
        azz[side, pl.ds(2 * base + many, many), :] = low
        k = FLAT.index((step_x, step_y))
        tzz[side, k] = table(cell, four, (-1, 1)[side], size_z, float(side * size_z), 8)

    _, own_planes, _, _, _ = PATCHES[0, 0]
    own_rows = own_planes * TALL

    def interpolate(field):
        high, low = split(field.reshape(3 * own_rows, lanes))
        z_high, z_low = thi[0], tlo[0]
        part = dot_nn(high, z_high) + dot_nn(low, z_high) + dot_nn(high, z_low)
        plane = txy[pl.ds(0, own_rows), :]
        return jnp.concatenate(
            [
                jnp.sum(part[c * own_rows : (c + 1) * own_rows] * plane, axis=0, keepdims=True)
                for c in range(3)
            ],
            axis=0,
        )

    def spread_main(turn, step_x, step_y):
        start, planes, first_row, rows, base = PATCHES[step_x, step_y]
        number = slots.index((step_x, step_y, 0))
        k = FLAT.index((step_x, step_y))
        plane = txy[pl.ds(base, planes * rows), :]
        high, low = split(
            jnp.concatenate([plane * joined(fbuf, turn - 1, number, c) for c in range(3)], axis=0)
        )
        part = dot_nt(high, thi[k]) + dot_nt(low, thi[k]) + dot_nt(high, tlo[k])
        part = part.reshape(3, planes, rows, lanes)
        if number == 0:
            for edge_plane in (0, WIDE - 1):
                grid[:, edge_plane] = jnp.zeros((3, TALL, lanes), jnp.float32)
            grid[:, pl.ds(start, planes)] = part
        else:
            grid[:, pl.ds(start, planes), pl.ds(first_row, rows)] += part

    def spread_side(turn, step_x, step_y, side):
        start, planes, first_row, rows, base = PATCHES[step_x, step_y]
        number = slots.index((step_x, step_y, (-1, 1)[side]))
        k = FLAT.index((step_x, step_y))
        many = planes * rows
        tab = tzz[side, k]
        pieces = [tab * joined(fbuf, turn - 1, number, c) for c in range(3)]
        high, low = split(jnp.concatenate(pieces + [jnp.zeros_like(tab)], axis=0))
        part = dot_nt(
            azz[side, pl.ds(2 * base, 2 * many), :], jnp.concatenate([high, low], axis=0)
        )
        part = (part[:many] + part[many:]).reshape(planes, rows, 64)
        where = (side, pl.ds(start, planes), pl.ds(first_row, rows), pl.ds(0, 64))
        if (step_x, step_y) == (0, 0):
            edge[where] = part
        else:
            edge[where] += part

    def finish_sides():
        inside = lax.broadcasted_iota(jnp.int32, (WIDE, TALL, size_z), 2) < 8
        for side in range(2):
            both = edge[side]
            both = both + turned(both, -32, 2)
            for c in range(3):
                part = jnp.where(inside, turned(both, -8 * c, 2), 0.0)
                grid[c, :, :, pl.ds(side * size_z, size_z)] += part

    def spread_rest(turn):
        wait_round(turn)
        for side in range(2):
            for edge_plane in (0, WIDE - 1):
                edge[side, edge_plane] = jnp.zeros((TALL, size_z), jnp.float32)
        for step_x, step_y in FLAT:
            if step_x or step_y:
                spread_main(turn, step_x, step_y)
        for side in range(2):
            for step_x, step_y in FLAT:
                spread_side(turn, step_x, step_y, side)
        finish_sides()

    def add(value, axis):
        return turned(value, -1, axis) + turned(value, 1, axis)

    def sub(value, axis):
        return turned(value, -1, axis) - turned(value, 1, axis)

    def respond():
        scale = fields[3]
        mx, my, mz = (scale * grid[c] for c in range(3))
        slope_y, slope_z = sub(my, 1), sub(mz, 2)
        sum_x = 2.0 * mx + add(mx, 1) + add(mx, 2)
        slope = slope_y + slope_z
        px = sum_x[2:] + sum_x[:-2] + slope[2:] - slope[:-2]
        slope_x = mx[2:] - mx[:-2]
        sum_y = (2.0 * my + add(my, 2))[1:-1] + my[2:] + my[:-2]
        tilt = slope_x + slope_z[1:-1]
        py = turned(sum_y + tilt, -1, 1) + turned(sum_y - tilt, 1, 1)
        sum_z = (2.0 * mz + add(mz, 1))[1:-1] + mz[2:] + mz[:-2]
        tilt = slope_x + slope_y[1:-1]
        pz = turned(sum_z + tilt, -1, 2) + turned(sum_z - tilt, 1, 2)
        half = scale[1:-1] * 0.5
        return jnp.stack(
            [half * (m[1:-1] + p * (1.0 / 12.0)) for m, p in ((mx, px), (my, py), (mz, pz))]
        )

    def apply(turn, vector):
        spread_rest(turn)
        return live * (interpolate(respond()) + stiffness * vector)

    left_half = lax.broadcasted_iota(jnp.int32, (1, 128), 1) < 64

    def partial_sums(residual, image):
        folded = []
        for other in (residual, image):
            line = jnp.sum(residual * other, axis=0, keepdims=True)
            total = line[:, :128]
            for at in range(128, cap, 128):
                total = total + line[:, at : at + 128]
            folded.append(total + turned(total, 64, 1))
        return jnp.where(left_half, folded[0], folded[1])

    def totals(tile):
        return (
            jnp.sum(jnp.where(left_half, tile, 0.0), axis=1, keepdims=True),
            jnp.sum(jnp.where(left_half, 0.0, tile), axis=1, keepdims=True),
        )

    loads[0].wait()
    pack(0)
    loads[2].wait()
    loads[3].wait()
    each = cap // 128
    for k, size in enumerate(sizes):
        local = (cells_ref[pl.ds(k, 1), :] - me[k] * size).astype(jnp.float32)
        for values, at in ((local, k), (offsets_ref[pl.ds(k, 1), :], k + 3)):
            for part in range(each):
                a, b = divmod(at * each + part, 4)
                nbuf[0, a, pl.ds(b, 1), :] = values[:, part * 128 : part * 128 + 128]
    loads[1].wait()
    pack(1)
    for load in loads[4:]:
        load.wait()
    pl.semaphore_wait(barrier, len(peers))
    go(halos(0))
    send_round(0)
    go(halos(1))
    target, stiffness = target_ref[...], stiffness_ref[...]
    live = (lax.broadcasted_iota(jnp.int32, (1, cap), 1) < count_ref[0]).astype(jnp.float32)
    build_main(0, 0)
    edge[...] = jnp.zeros_like(edge)
    wait_halos(0)
    widen(0)
    base = live * (target - interpolate(fields[pl.ds(0, 3), pl.ds(1, own_planes)]))
    put(1, base)
    send_round(1)
    spread_main(1, 0, 0)
    wait_round(0)
    for step_x, step_y in FLAT:
        if step_x or step_y:
            build_main(step_x, step_y)
        build_side(step_x, step_y, 0)
        build_side(step_x, step_y, 1)
    wait_halos(1)
    widen(1)
    first = apply(1, base)
    send_sum("near", partial_sums(base, first))
    put(2, first)
    send_round(2)
    spread_main(2, 0, 0)
    send_sum("far", wait_sum("near"))
    second = apply(2, first)
    put(3, second)
    send_round(3)
    spread_main(3, 0, 0)
    norm, product = totals(wait_sum("far"))
    alpha = norm / product
    answer = alpha * base
    residual, image = base - alpha * first, first - alpha * second
    send_sum(1, partial_sums(residual, image))
    third = apply(3, second)
    again = second - alpha * third
    norm_before, alpha_before = norm, alpha
    norm, product = totals(wait_sum(1))
    ratio = norm / norm_before
    alpha = norm / (product - ratio * norm / alpha_before)
    direction = residual + ratio * base
    answer = answer + alpha * direction
    residual, image = (
        residual - alpha * (image + ratio * first),
        image - alpha * (again + ratio * second),
    )
    send_sum(2, partial_sums(residual, image))
    norm_before, alpha_before = norm, alpha
    norm, product = totals(wait_sum(2))
    ratio = norm / norm_before
    alpha = norm / (product - ratio * norm / alpha_before)
    out[...] = answer + alpha * (residual + ratio * direction)
    for copy in sent:
        copy.wait_send()


def body(mesh_counts, density, base_velocity, cells, offsets, target, stiffness, counts):
    sizes = density.shape
    size_x, size_y, size_z = sizes
    cap = cells.shape[1]
    assert sizes == (8, 8, 128) and min(mesh_counts) > 2
    lanes = 2 * size_z
    number, flat = 27, 9
    turns = ITERS + 1
    halo_shapes = []
    for parts, low, high, slot in KINDS:
        more = -(-high * slot // size_y)
        halo_shapes += [(len(parts), low), (len(parts), slot), (), (), (len(parts), low + high)]
        halo_shapes += [(len(parts), low + 2), (len(parts), slot + 1 + more), (2, flat)]
    near, far = mesh_counts[1] * mesh_counts[2], mesh_counts[0]
    return pl.pallas_call(
        functools.partial(kernel, mesh_counts, sizes),
        out_shape=jax.ShapeDtypeStruct((3, cap), jnp.float32),
        in_specs=[pl.BlockSpec(memory_space=pltpu.HBM)] * 7,
        out_specs=pl.BlockSpec(memory_space=pltpu.VMEM),
        scratch_shapes=[
            pltpu.VMEM((4, size_x, size_y, size_z), jnp.float32),
            pltpu.VMEM((3, cap), jnp.int32),
            pltpu.VMEM((3, cap), jnp.float32),
            pltpu.VMEM((3, cap), jnp.float32),
            pltpu.VMEM((1, cap), jnp.float32),
            pltpu.SMEM((1,), jnp.int32),
            pltpu.VMEM((4, WIDE, TALL, lanes), jnp.float32),
            *[pltpu.VMEM(shape + (size_y, size_z), jnp.float32) for shape in halo_shapes],
            pltpu.VMEM((number, 3 * (cap // 256), 4, 128), jnp.float32),
            pltpu.VMEM((ITERS, number, 3, cap // 128, 128), jnp.float32),
            pltpu.VMEM((1, near, 1, 128), jnp.float32),
            pltpu.VMEM((1, far, 1, 128), jnp.float32),
            pltpu.VMEM((2, near * far, 1, 128), jnp.float32),
            pltpu.VMEM((PATCH_ROWS, cap), jnp.float32),
            pltpu.VMEM((flat, lanes, cap), jnp.bfloat16),
            pltpu.VMEM((flat, lanes, cap), jnp.bfloat16),
            pltpu.VMEM((2, 2 * PATCH_ROWS, cap), jnp.bfloat16),
            pltpu.VMEM((2, flat, 8, cap), jnp.float32),
            pltpu.VMEM((2, WIDE, TALL, size_z), jnp.float32),
            pltpu.VMEM((3, WIDE, TALL, lanes), jnp.float32),
            pltpu.SemaphoreType.DMA((7,)),
            pltpu.SemaphoreType.DMA((turns,)),
            pltpu.SemaphoreType.DMA((turns,)),
            pltpu.SemaphoreType.DMA((4,)),
            pltpu.SemaphoreType.DMA((4,)),
            pltpu.SemaphoreType.DMA((8,)),
            pltpu.SemaphoreType.DMA((8,)),
        ],
        compiler_params=pltpu.CompilerParams(
            collective_id=0, has_side_effects=True, vmem_limit_bytes=60 * 1024 * 1024
        ),
    )(density, base_velocity, cells, offsets, target, stiffness[None], counts)


def solution(mesh):
    return jax.shard_map(
        functools.partial(body, tuple(mesh.shape[name] for name in AXES)),
        mesh=mesh,
        in_specs=(
            P("gx", "gy", "gz"),
            P(None, "gx", "gy", "gz"),
            P(None, ("gx", "gy", "gz")),
            P(None, ("gx", "gy", "gz")),
            P(None, ("gx", "gy", "gz")),
            P(("gx", "gy", "gz")),
            P(("gx", "gy", "gz")),
        ),
        out_specs=P(None, ("gx", "gy", "gz")),
        check_vma=False,
    )
```

```python
import functools
import itertools

import jax
import jax.numpy as jnp
from jax import lax
from jax.experimental import pallas as pl
from jax.experimental.pallas import tpu as pltpu
from jax.sharding import PartitionSpec as P

ITERS = 3
LOW = 2
KINDS = (((0, 1, 2), 1, 2, 2), ((3,), 2, 3, 4))
WIDE, TALL, HALF = 13, 16, 8
STEPS = (0, -1, 1)
MESH_ID = pl.DeviceIdType.MESH
AXES = ("gx", "gy", "gz")


def round_up(value, multiple):
    return -(-value // multiple) * multiple


def span(shift, size):
    return {0: (1, size + 3), -1: (0, 4), 1: (size + 1, 4)}[shift]


def weights(fraction):
    root = jnp.sqrt(1.0 + 4.0 * fraction - 4.0 * fraction * fraction)
    near, far = 3.0 - 2.0 * fraction, 1.0 + 2.0 * fraction
    return ((near - root) / 8.0, (near + root) / 8.0, (far + root) / 8.0, (far - root) / 8.0)


def table(cell, four, shift, size, first, rows):
    place = lax.broadcasted_iota(jnp.int32, (rows, cell.shape[1]), 0).astype(jnp.float32) + first
    apart = place - (cell + (1.0 + shift * size))
    total = jnp.where(apart == 3.0, four[3], 0.0)
    for number in (2, 1, 0):
        total = jnp.where(apart == float(number), four[number], total)
    return total


def split(value):
    high = value.astype(jnp.bfloat16)
    return high, (value - high.astype(jnp.float32)).astype(jnp.bfloat16)


def dot_nt(a, b):
    return lax.dot_general(a, b, (((1,), (1,)), ((), ())), preferred_element_type=jnp.float32)


def dot_nn(a, b):
    return lax.dot_general(a, b, (((1,), (0,)), ((), ())), preferred_element_type=jnp.float32)


def patches():
    found, base = {}, 0
    for step_x, step_y in itertools.product(STEPS, STEPS):
        row, rows = {0: (0, TALL), -1: (0, HALF), 1: (HALF, HALF)}[step_y]
        start, planes = span(step_x, 8)
        if step_x == 0 and step_y:
            planes += 1
        found[step_x, step_y] = (start, planes, row, rows, base)
        base += planes * rows
    return found, base


PATCHES, PATCH_ROWS = patches()
FLAT = list(PATCHES)


def kernel(
    counts, sizes, density, velocity, cells_in, offsets_in, target_in, stiffness_in, count_in, out,
    block, cells_ref, offsets_ref, target_ref, stiffness_ref, count_ref,
    fields, low_v, high_v, start_v, end_v, x_v, below_v, above_v, z_v,
    low_d, high_d, start_d, end_d, x_d, below_d, above_d, z_d, nbuf, fbuf, rbuf, sbuf, dbuf,
    txy, thi, tlo, azz, tzz, edge, grid,
    lsem, nsend, nrecv, ssend, srecv, hsend, hrecv,
):
    size_x, size_y, size_z = sizes
    cap = cells_ref.shape[1]
    lanes = fields.shape[3]
    slots = list(itertools.product(STEPS, STEPS, STEPS))
    me = [lax.axis_index(name) for name in AXES]
    sent = []
    packs = ((low_v, high_v, start_v, end_v), (low_d, high_d, start_d, end_d))
    landing = ((x_v, below_v, above_v, z_v), (x_d, below_d, above_d, z_d))

    def device(offset):
        return tuple(lax.rem(m + (o % n), n) for m, o, n in zip(me, offset, counts))

    def negated(offset):
        return tuple(-o for o in offset)

    near = [o for o in itertools.product([0], range(counts[1]), range(counts[2])) if any(o)]
    far = [(o, 0, 0) for o in range(1, counts[0])]
    whole = [o for o in itertools.product(*[range(n) for n in counts]) if any(o)]
    wrapped = {tuple(o % n for o, n in zip(slot, counts)) for slot in slots if any(slot)}
    half_way = {(counts[0] // 2, 0, 0), (0, counts[1] // 2, 0)}
    peers = sorted(wrapped | half_way)
    loads = [
        pltpu.make_async_copy(source, destination, lsem.at[k])
        for k, (source, destination) in enumerate(
            [
                (velocity, block.at[pl.ds(0, 3)]),
                (density, block.at[3]),
                (cells_in, cells_ref),
                (offsets_in, offsets_ref),
                (target_in, target_ref),
                (stiffness_in, stiffness_ref),
                (count_in, count_ref),
            ]
        )
    ]
    barrier = pltpu.get_barrier_semaphore()
    for peer in peers:
        pl.semaphore_signal(barrier, inc=1, device_id=device(peer), device_id_type=MESH_ID)
    for load in loads:
        load.start()

    def go(copies):
        for copy in copies:
            copy.start()

    def every(ref, send, receive):
        copy = pltpu.make_async_remote_copy(
            src_ref=ref,
            dst_ref=ref,
            send_sem=send,
            recv_sem=receive,
            device_id=device(far[0]),
            device_id_type=MESH_ID,
        )
        sent.append(copy)
        return copy

    def neighbour_copy(turn, number):
        return pltpu.make_async_remote_copy(
            src_ref=fbuf.at[turn - 1, 0] if turn else nbuf.at[0],
            dst_ref=fbuf.at[turn - 1, number] if turn else nbuf.at[number],
            send_sem=nsend.at[turn],
            recv_sem=nrecv.at[turn],
            device_id=device(negated(slots[number])),
            device_id_type=MESH_ID,
        )

    def send_round(turn):
        far_first = sorted(range(1, len(slots)), key=lambda k: (-sum(map(abs, slots[k])), k))
        go([neighbour_copy(turn, number) for number in far_first])

    def wait_round(turn):
        others = pl.ds(1, len(slots) - 1)
        landed = fbuf.at[turn - 1, others] if turn else nbuf.at[others]
        every(landed, nsend.at[turn], nrecv.at[turn]).wait_recv()

    def away(offset):
        return sum(min(o, n - o) for o, n in zip(offset, counts))

    stages = {
        "near": (near, rbuf.at[0], ssend.at[0], srecv.at[0]),
        "far": (far, sbuf.at[0], ssend.at[1], srecv.at[1]),
        1: (whole, dbuf.at[0], ssend.at[2], srecv.at[2]),
        2: (whole, dbuf.at[1], ssend.at[3], srecv.at[3]),
    }

    def send_sum(stage, value):
        members, buffer, send, receive = stages[stage]
        buffer[0] = value
        for number in sorted(range(len(members)), key=lambda k: (-away(members[k]), k)):
            pltpu.make_async_remote_copy(
                src_ref=buffer.at[0],
                dst_ref=buffer.at[number + 1],
                send_sem=send,
                recv_sem=receive,
                device_id=device(negated(members[number])),
                device_id_type=MESH_ID,
            ).start()

    def wait_sum(stage):
        members, buffer, send, receive = stages[stage]
        every(buffer.at[pl.ds(1, len(members))], send, receive).wait_recv()
        total = buffer[...]
        while total.shape[0] > 1:
            half = total.shape[0] // 2
            total = total[:half] + total[half:]
        return total[0]

    def put(turn, vector):
        for c in range(3):
            for part in range(cap // 128):
                fbuf[turn - 1, 0, c, pl.ds(part, 1), :] = vector[
                    c : c + 1, part * 128 : part * 128 + 128
                ]

    def joined(ref, at, number, k):
        return jnp.concatenate(
            [ref[at, number, k, pl.ds(part, 1), :] for part in range(cap // 128)], axis=1
        )

    def mark(number, k):
        each = cap // 128
        parts = [divmod(k * each + part, 4) for part in range(each)]
        return jnp.concatenate([nbuf[number, a, pl.ds(b, 1), :] for a, b in parts], axis=1)

    def halo_copy(number, source, target, step):
        return pltpu.make_async_remote_copy(
            src_ref=source,
            dst_ref=target,
            send_sem=hsend.at[number],
            recv_sem=hrecv.at[number],
            device_id=device(negated(step)),
            device_id_type=MESH_ID,
        )

    corners_first = sorted(FLAT, key=lambda o: -abs(o[0]) - abs(o[1]))

    def halos(kind):
        parts, low, high, slot = KINDS[kind]
        (source_x, source_low, source_high, source_start, source_end), targets = (
            (block.at[pl.ds(parts[0], len(parts))], *packs[kind]),
            landing[kind],
        )
        more = -(-high * slot // size_y)
        spaces = (
            (source_x, targets[0], {-1: (size_x - low, low, 0), 1: (0, high, low)}),
            (source_low, targets[1], {-1: (low - 1, 1, 0), 0: (0, low, 1), 1: (0, 1, low + 1)}),
            (source_high, targets[2], {-1: (slot - 1, 1, 0), 0: (0, slot, 1), 1: (0, more, slot + 1)}),
        )
        copies = []
        for step_x, step_y in corners_first:
            if step_x or step_y:
                space = 0 if step_y == 0 else 1 if step_y < 0 else 2
                source, target, where = spaces[space]
                first, many, at = where[step_x]
                copies.append(
                    halo_copy(
                        4 * kind + space,
                        source.at[:, pl.ds(first, many)],
                        target.at[:, pl.ds(at, many)],
                        (step_x, step_y, 0),
                    )
                )
        for step_x, step_y in corners_first:
            for side, step_z in enumerate((-1, 1)):
                copies.append(
                    halo_copy(
                        4 * kind + 3,
                        (source_start, source_end)[side],
                        targets[3].at[side, FLAT.index((step_x, step_y))],
                        (step_x, step_y, step_z),
                    )
                )
        return copies

    def wait_halos(kind):
        for space, target in enumerate(landing[kind]):
            at = 4 * kind + space
            every(target, hsend.at[at], hrecv.at[at]).wait_recv()

    lane = lax.broadcasted_iota(jnp.int32, (size_y, size_z), 1)
    row = lax.broadcasted_iota(jnp.int32, (size_y, size_z), 0)

    def turned(value, by, axis):
        by %= value.shape[axis]
        return pltpu.roll(value, by, axis) if by else value

    def pack(kind):
        parts, low, high, slot = KINDS[kind]
        source_low, source_high, source_start, source_end = packs[kind]
        starts = [jnp.zeros((size_y, size_z), jnp.float32)] * 2
        ends = [jnp.zeros((size_y, size_z), jnp.float32)] * 2
        for i, c in enumerate(parts):
            tiles_low, tiles_high = [None] * low, [None] * slot
            for plane in range(size_x):
                own = block[c, plane]
                t, q = divmod(plane, size_y // low)
                moved = turned(own, low * (q + 1) - size_y, 0)
                tiles_low[t] = moved if q == 0 else jnp.where(row // low == q, moved, tiles_low[t])
                t, q = divmod(plane, size_y // slot)
                moved = turned(own, slot * q, 0)
                tiles_high[t] = moved if q == 0 else jnp.where(row // slot == q, moved, tiles_high[t])
                at = i * size_x + plane
                chain = plane % 2
                starts[chain] = jnp.where(
                    lane // low == at, turned(own, low * (at + 1) - size_z, 1), starts[chain]
                )
                ends[chain] = jnp.where(lane // slot == at, turned(own, slot * at, 1), ends[chain])
            for t in range(low):
                source_low[i, t] = tiles_low[t]
            for t in range(slot):
                source_high[i, t] = tiles_high[t]
        source_start[...] = jnp.where(lane // low % 2 == 0, starts[0], starts[1])
        source_end[...] = jnp.where(lane // slot % 2 == 0, ends[0], ends[1])

    def tall_of(down, own, up):
        moved = turned(own, LOW, 0)
        return jnp.where(row < LOW, down, moved), jnp.where(row < LOW, moved, up)

    def widen(kind):
        parts, low, high, slot = KINDS[kind]
        xbuf, below, above, zbuf = landing[kind]
        blank = 1.0 if kind else 0.0
        sides = {}
        for step_x in STEPS:
            for side in range(2):
                down, own, up = (zbuf[side, FLAT.index((step_x, step_y))] for step_y in (-1, 0, 1))
                sides[step_x, side] = tall_of(turned(down, LOW, 0), own, turned(up, LOW, 0))
        for x in range(-low, size_x + high):
            step_x = -1 if x < 0 else 0 if x < size_x else 1
            inner = x - step_x * size_x
            for i, c in enumerate(parts):
                own = block[c, x] if step_x == 0 else xbuf[i, x + low if step_x < 0 else x - size_x + low]
                t, q = divmod(inner, size_y // low)
                t = (0, t + 1, low + 1)[step_x + 1]
                down = turned(below[i, t], LOW - low * (q + 1), 0)
                t, q = divmod(inner, size_y // slot)
                t = (0, t + 1, t + slot + 1)[step_x + 1]
                up = turned(above[i, t], LOW - slot * q, 0)
                if low < LOW:
                    down = jnp.where(row >= LOW - low, down, blank)
                talls = tall_of(down, own, jnp.where(row < LOW + high, up, blank))
                at = i * size_x + inner
                for half in range(2):
                    moved = turned(talls[half], LOW, 1)
                    start = turned(sides[step_x, 0][half], LOW - low * (at + 1), 1)
                    end = turned(sides[step_x, 1][half], LOW - slot * at, 1)
                    if low < LOW:
                        start = jnp.where(lane >= LOW - low, start, blank)
                    left = jnp.where(lane < LOW, start, moved)
                    right = jnp.where(lane < LOW, moved, jnp.where(lane < LOW + high, end, blank))
                    if half:
                        left = jnp.where(row < LOW + high, left, blank)
                        right = jnp.where(row < LOW + high, right, blank)
                    if kind:
                        left, right = lax.rsqrt(left), lax.rsqrt(right)
                    rows = pl.ds(half * size_y, size_y)
                    fields[c, x + LOW, rows, pl.ds(0, size_z)] = left
                    fields[c, x + LOW, rows, pl.ds(size_z, size_z)] = right

    def tables(step_x, step_y, step_z):
        number = slots.index((step_x, step_y, step_z))
        cells = [mark(number, k) for k in range(3)]
        fours = [weights(mark(number, k + 3)) for k in range(3)]
        start, planes, first_row, rows, base = PATCHES[step_x, step_y]
        first = start // 8 * 8
        tall = round_up(start + planes - first, 8)
        tab_x = table(cells[0], fours[0], step_x, size_x, float(first), tall)
        tab_y = table(cells[1], fours[1], step_y, size_y, float(first_row), rows)
        return cells[2], fours[2], [
            tab_x[start - first + plane : start - first + plane + 1] * tab_y for plane in range(planes)
        ]

    def build_main(step_x, step_y):
        cell, four, products = tables(step_x, step_y, 0)
        start, planes, first_row, rows, base = PATCHES[step_x, step_y]
        for plane, product in enumerate(products):
            txy[pl.ds(base + plane * rows, rows), :] = product
        k = FLAT.index((step_x, step_y))
        high, low = split(table(cell, four, 0, size_z, 0.0, used))
        for ref, part in ((thi, high), (tlo, low)):
            ref[k, pl.ds(0, used), :] = part
            ref[k, pl.ds(used, lanes - used), :] = jnp.zeros((lanes - used, cap), jnp.bfloat16)

    def build_side(step_x, step_y, side):
        cell, four, products = tables(step_x, step_y, (-1, 1)[side])
        start, planes, first_row, rows, base = PATCHES[step_x, step_y]
        many = planes * rows
        high, low = split(jnp.concatenate(products, axis=0))
        azz[side, pl.ds(2 * base, many), :] = high
        azz[side, pl.ds(2 * base + many, many), :] = low
        k = FLAT.index((step_x, step_y))
        tzz[side, k] = table(cell, four, (-1, 1)[side], size_z, float(side * size_z), 8)

    own_planes = PATCHES[0, 0][1]
    own_rows = own_planes * TALL
    used = round_up(size_z + 5, 16)

    def interpolate(field):
        high, low = split(field.reshape(3 * own_rows, lanes))
        z_high, z_low = thi[0], tlo[0]
        part = dot_nn(high, z_high) + dot_nn(low, z_high) + dot_nn(high, z_low)
        plane = txy[pl.ds(0, own_rows), :]
        return jnp.concatenate(
            [
                jnp.sum(part[c * own_rows : (c + 1) * own_rows] * plane, axis=0, keepdims=True)
                for c in range(3)
            ],
            axis=0,
        )

    def spread_main(turn, step_x, step_y):
        start, planes, first_row, rows, base = PATCHES[step_x, step_y]
        number = slots.index((step_x, step_y, 0))
        k = FLAT.index((step_x, step_y))
        plane = txy[pl.ds(base, planes * rows), :]
        high, low = split(
            jnp.concatenate([plane * joined(fbuf, turn - 1, number, c) for c in range(3)], axis=0)
        )
        z_high, z_low = thi[k, pl.ds(0, used), :], tlo[k, pl.ds(0, used), :]
        part = dot_nt(high, z_high) + dot_nt(low, z_high) + dot_nt(high, z_low)
        part = part.reshape(3, planes, rows, used)
        if number == 0:
            for edge_plane in (0, WIDE - 1):
                grid[:, edge_plane] = jnp.zeros((3, TALL, lanes), jnp.float32)
            grid[:, pl.ds(start, planes), :, pl.ds(0, used)] = part
        else:
            grid[:, pl.ds(start, planes), pl.ds(first_row, rows), pl.ds(0, used)] += part

    def spread_side(turn, step_x, step_y, side):
        start, planes, first_row, rows, base = PATCHES[step_x, step_y]
        number = slots.index((step_x, step_y, (-1, 1)[side]))
        k = FLAT.index((step_x, step_y))
        many = planes * rows
        tab = tzz[side, k]
        pieces = [tab * joined(fbuf, turn - 1, number, c) for c in range(3)]
        high, low = split(jnp.concatenate(pieces + [jnp.zeros_like(tab)], axis=0))
        part = dot_nt(
            azz[side, pl.ds(2 * base, 2 * many), :], jnp.concatenate([high, low], axis=0)
        )
        part = (part[:many] + part[many:]).reshape(planes, rows, 64)
        where = (side, pl.ds(start, planes), pl.ds(first_row, rows), pl.ds(0, 64))
        if (step_x, step_y) == (0, 0):
            edge[where] = part
        else:
            edge[where] += part

    def finish_sides():
        inside = lax.broadcasted_iota(jnp.int32, (WIDE, TALL, size_z), 2) < 8
        for side in range(2):
            both = edge[side]
            both = both + turned(both, -32, 2)
            for c in range(3):
                part = jnp.where(inside, turned(both, -8 * c, 2), 0.0)
                grid[c, :, :, pl.ds(side * size_z, size_z)] += part

    def spread_rest(turn):
        wait_round(turn)
        for side in range(2):
            for edge_plane in (0, WIDE - 1):
                edge[side, edge_plane] = jnp.zeros((TALL, size_z), jnp.float32)
        for step_x, step_y in FLAT:
            for side in range(2):
                spread_side(turn, step_x, step_y, side)
        for step_x, step_y in FLAT:
            if step_x or step_y:
                spread_main(turn, step_x, step_y)
        finish_sides()

    def add(value, axis):
        return turned(value, -1, axis) + turned(value, 1, axis)

    def sub(value, axis):
        return turned(value, -1, axis) - turned(value, 1, axis)

    def respond():
        scale = fields[3]
        mx, my, mz = (scale * grid[c] for c in range(3))
        slope_y, slope_z = sub(my, 1), sub(mz, 2)
        sum_x = 2.0 * mx + add(mx, 1) + add(mx, 2)
        slope = slope_y + slope_z
        px = sum_x[2:] + sum_x[:-2] + slope[2:] - slope[:-2]
        slope_x = mx[2:] - mx[:-2]
        sum_y = (2.0 * my + add(my, 2))[1:-1] + my[2:] + my[:-2]
        tilt = slope_x + slope_z[1:-1]
        py = turned(sum_y + tilt, -1, 1) + turned(sum_y - tilt, 1, 1)
        sum_z = (2.0 * mz + add(mz, 1))[1:-1] + mz[2:] + mz[:-2]
        tilt = slope_x + slope_y[1:-1]
        pz = turned(sum_z + tilt, -1, 2) + turned(sum_z - tilt, 1, 2)
        half = scale[1:-1] * 0.5
        return jnp.stack(
            [half * (m[1:-1] + p * (1.0 / 12.0)) for m, p in ((mx, px), (my, py), (mz, pz))]
        )

    def apply(turn, vector):
        spread_rest(turn)
        return live * (interpolate(respond()) + stiffness * vector)

    left_half = lax.broadcasted_iota(jnp.int32, (1, 128), 1) < 64

    def partial_sums(residual, image):
        folded = []
        for other in (residual, image):
            line = jnp.sum(residual * other, axis=0, keepdims=True)
            total = line[:, :128]
            for at in range(128, cap, 128):
                total = total + line[:, at : at + 128]
            folded.append(total + turned(total, 64, 1))
        return jnp.where(left_half, folded[0], folded[1])

    def totals(tile):
        return (
            jnp.sum(jnp.where(left_half, tile, 0.0), axis=1, keepdims=True),
            jnp.sum(jnp.where(left_half, 0.0, tile), axis=1, keepdims=True),
        )

    loads[0].wait()
    pack(0)
    pl.semaphore_wait(barrier, len(peers))
    go(halos(0))
    loads[2].wait()
    loads[3].wait()
    each = cap // 128
    for k, size in enumerate(sizes):
        local = (cells_ref[pl.ds(k, 1), :] - me[k] * size).astype(jnp.float32)
        for values, at in ((local, k), (offsets_ref[pl.ds(k, 1), :], k + 3)):
            for part in range(each):
                a, b = divmod(at * each + part, 4)
                nbuf[0, a, pl.ds(b, 1), :] = values[:, part * 128 : part * 128 + 128]
    send_round(0)
    loads[1].wait()
    pack(1)
    go(halos(1))
    for load in loads[4:]:
        load.wait()
    target, stiffness = target_ref[...], stiffness_ref[...]
    live = (lax.broadcasted_iota(jnp.int32, (1, cap), 1) < count_ref[0]).astype(jnp.float32)
    build_main(0, 0)
    edge[...] = jnp.zeros_like(edge)
    grid[...] = jnp.zeros_like(grid)
    wait_halos(0)
    widen(0)
    base = live * (target - interpolate(fields[pl.ds(0, 3), pl.ds(1, own_planes)]))
    put(1, base)
    send_round(1)
    spread_main(1, 0, 0)
    wait_round(0)
    for step_x, step_y in FLAT:
        if step_x or step_y:
            build_main(step_x, step_y)
        build_side(step_x, step_y, 0)
        build_side(step_x, step_y, 1)
    wait_halos(1)
    widen(1)
    first = apply(1, base)
    send_sum("near", partial_sums(base, first))
    put(2, first)
    send_round(2)
    spread_main(2, 0, 0)
    send_sum("far", wait_sum("near"))
    second = apply(2, first)
    put(3, second)
    send_round(3)
    spread_main(3, 0, 0)
    norm, product = totals(wait_sum("far"))
    alpha = norm / product
    answer = alpha * base
    residual, image = base - alpha * first, first - alpha * second
    send_sum(1, partial_sums(residual, image))
    third = apply(3, second)
    again = second - alpha * third
    norm_before, alpha_before = norm, alpha
    norm, product = totals(wait_sum(1))
    ratio = norm / norm_before
    alpha = norm / (product - ratio * norm / alpha_before)
    direction = residual + ratio * base
    answer = answer + alpha * direction
    residual, image = (
        residual - alpha * (image + ratio * first),
        image - alpha * (again + ratio * second),
    )
    send_sum(2, partial_sums(residual, image))
    norm_before, alpha_before = norm, alpha
    norm, product = totals(wait_sum(2))
    ratio = norm / norm_before
    alpha = norm / (product - ratio * norm / alpha_before)
    out[...] = answer + alpha * (residual + ratio * direction)
    for copy in sent:
        copy.wait_send()


def body(mesh_counts, density, base_velocity, cells, offsets, target, stiffness, counts):
    sizes = density.shape
    size_x, size_y, size_z = sizes
    cap = cells.shape[1]
    assert sizes == (8, 8, 128) and min(mesh_counts) > 2
    lanes = 2 * size_z
    number, flat = 27, 9
    turns = ITERS + 1
    halo_shapes = []
    for parts, low, high, slot in KINDS:
        more = -(-high * slot // size_y)
        halo_shapes += [(len(parts), low), (len(parts), slot), (), (), (len(parts), low + high)]
        halo_shapes += [(len(parts), low + 2), (len(parts), slot + 1 + more), (2, flat)]
    near, far = mesh_counts[1] * mesh_counts[2], mesh_counts[0]
    return pl.pallas_call(
        functools.partial(kernel, mesh_counts, sizes),
        out_shape=jax.ShapeDtypeStruct((3, cap), jnp.float32),
        in_specs=[pl.BlockSpec(memory_space=pltpu.HBM)] * 7,
        out_specs=pl.BlockSpec(memory_space=pltpu.VMEM),
        scratch_shapes=[
            pltpu.VMEM((4, size_x, size_y, size_z), jnp.float32),
            pltpu.VMEM((3, cap), jnp.int32),
            pltpu.VMEM((3, cap), jnp.float32),
            pltpu.VMEM((3, cap), jnp.float32),
            pltpu.VMEM((1, cap), jnp.float32),
            pltpu.SMEM((1,), jnp.int32),
            pltpu.VMEM((4, WIDE, TALL, lanes), jnp.float32),
            *[pltpu.VMEM(shape + (size_y, size_z), jnp.float32) for shape in halo_shapes],
            pltpu.VMEM((number, 3 * (cap // 256), 4, 128), jnp.float32),
            pltpu.VMEM((ITERS, number, 3, cap // 128, 128), jnp.float32),
            pltpu.VMEM((1, near, 1, 128), jnp.float32),
            pltpu.VMEM((1, far, 1, 128), jnp.float32),
            pltpu.VMEM((2, near * far, 1, 128), jnp.float32),
            pltpu.VMEM((PATCH_ROWS, cap), jnp.float32),
            pltpu.VMEM((flat, lanes, cap), jnp.bfloat16),
            pltpu.VMEM((flat, lanes, cap), jnp.bfloat16),
            pltpu.VMEM((2, 2 * PATCH_ROWS, cap), jnp.bfloat16),
            pltpu.VMEM((2, flat, 8, cap), jnp.float32),
            pltpu.VMEM((2, WIDE, TALL, size_z), jnp.float32),
            pltpu.VMEM((3, WIDE, TALL, lanes), jnp.float32),
            pltpu.SemaphoreType.DMA((7,)),
            pltpu.SemaphoreType.DMA((turns,)),
            pltpu.SemaphoreType.DMA((turns,)),
            pltpu.SemaphoreType.DMA((4,)),
            pltpu.SemaphoreType.DMA((4,)),
            pltpu.SemaphoreType.DMA((8,)),
            pltpu.SemaphoreType.DMA((8,)),
        ],
        compiler_params=pltpu.CompilerParams(
            collective_id=0, has_side_effects=True, vmem_limit_bytes=60 * 1024 * 1024
        ),
    )(density, base_velocity, cells, offsets, target, stiffness[None], counts)


def solution(mesh):
    return jax.shard_map(
        functools.partial(body, tuple(mesh.shape[name] for name in AXES)),
        mesh=mesh,
        in_specs=(
            P("gx", "gy", "gz"),
            P(None, "gx", "gy", "gz"),
            P(None, ("gx", "gy", "gz")),
            P(None, ("gx", "gy", "gz")),
            P(None, ("gx", "gy", "gz")),
            P(("gx", "gy", "gz")),
            P(("gx", "gy", "gz")),
        ),
        out_specs=P(None, ("gx", "gy", "gz")),
        check_vma=False,
    )
```

```python
import functools
import itertools

import jax
import jax.numpy as jnp
from jax import lax
from jax.experimental import pallas as pl
from jax.experimental.pallas import tpu as pltpu
from jax.sharding import PartitionSpec as P

ITERS = 3
LOW = 2
KINDS = (((0, 1, 2), 1, 2, 2), ((3,), 2, 3, 4))
WIDE, TALL, HALF = 13, 16, 8
STEPS = (0, -1, 1)
MESH_ID = pl.DeviceIdType.MESH
AXES = ("gx", "gy", "gz")


def round_up(value, multiple):
    return -(-value // multiple) * multiple


def span(shift, size):
    return {0: (1, size + 3), -1: (0, 4), 1: (size + 1, 4)}[shift]


def weights(fraction):
    root = jnp.sqrt(1.0 + 4.0 * fraction - 4.0 * fraction * fraction)
    near, far = 3.0 - 2.0 * fraction, 1.0 + 2.0 * fraction
    return ((near - root) / 8.0, (near + root) / 8.0, (far + root) / 8.0, (far - root) / 8.0)


def table(cell, four, shift, size, first, rows):
    place = lax.broadcasted_iota(jnp.int32, (rows, cell.shape[1]), 0).astype(jnp.float32) + first
    apart = place - (cell + (1.0 + shift * size))
    total = jnp.where(apart == 3.0, four[3], 0.0)
    for number in (2, 1, 0):
        total = jnp.where(apart == float(number), four[number], total)
    return total


def split(value):
    high = value.astype(jnp.bfloat16)
    return high, (value - high.astype(jnp.float32)).astype(jnp.bfloat16)


def dot_nt(a, b):
    return lax.dot_general(a, b, (((1,), (1,)), ((), ())), preferred_element_type=jnp.float32)


def dot_nn(a, b):
    return lax.dot_general(a, b, (((1,), (0,)), ((), ())), preferred_element_type=jnp.float32)


def patches():
    found, base = {}, 0
    for step_x, step_y in itertools.product(STEPS, STEPS):
        row, rows = {0: (0, TALL), -1: (0, HALF), 1: (HALF, HALF)}[step_y]
        start, planes = span(step_x, 8)
        if step_x == 0 and step_y:
            planes += 1
        found[step_x, step_y] = (start, planes, row, rows, base)
        base += planes * rows
    return found, base


PATCHES, PATCH_ROWS = patches()
FLAT = list(PATCHES)


def kernel(
    counts, sizes, density, velocity, cells_in, offsets_in, target_in, stiffness_in, count_in, out,
    block, cells_ref, offsets_ref, target_ref, stiffness_ref, count_ref,
    fields, low_v, high_v, start_v, end_v, x_v, below_v, above_v, z_v,
    low_d, high_d, start_d, end_d, x_d, below_d, above_d, z_d, nbuf, fbuf, rbuf, sbuf, dbuf,
    txy, thi, tlo, azz, tzz, edge, grid,
    lsem, nsend, nrecv, ssend, srecv, hsend, hrecv,
):
    size_x, size_y, size_z = sizes
    cap = cells_ref.shape[1]
    lanes = fields.shape[3]
    slots = list(itertools.product(STEPS, STEPS, STEPS))
    me = [lax.axis_index(name) for name in AXES]
    sent = []
    packs = ((low_v, high_v, start_v, end_v), (low_d, high_d, start_d, end_d))
    landing = ((x_v, below_v, above_v, z_v), (x_d, below_d, above_d, z_d))

    def device(offset):
        return tuple(lax.rem(m + (o % n), n) for m, o, n in zip(me, offset, counts))

    def negated(offset):
        return tuple(-o for o in offset)

    near = [o for o in itertools.product([0], range(counts[1]), range(counts[2])) if any(o)]
    far = [(o, 0, 0) for o in range(1, counts[0])]
    whole = [o for o in itertools.product(*[range(n) for n in counts]) if any(o)]
    wrapped = {tuple(o % n for o, n in zip(slot, counts)) for slot in slots if any(slot)}
    half_way = {(counts[0] // 2, 0, 0), (0, counts[1] // 2, 0)}
    peers = sorted(wrapped | half_way)
    loads = [
        pltpu.make_async_copy(source, destination, lsem.at[k])
        for k, (source, destination) in enumerate(
            [
                (velocity, block.at[pl.ds(0, 3)]),
                (density, block.at[3]),
                (cells_in, cells_ref),
                (offsets_in, offsets_ref),
                (target_in, target_ref),
                (stiffness_in, stiffness_ref),
                (count_in, count_ref),
            ]
        )
    ]
    barrier = pltpu.get_barrier_semaphore()
    for peer in peers:
        pl.semaphore_signal(barrier, inc=1, device_id=device(peer), device_id_type=MESH_ID)
    for load in loads:
        load.start()

    def go(copies):
        for copy in copies:
            copy.start()

    def every(ref, send, receive):
        copy = pltpu.make_async_remote_copy(
            src_ref=ref,
            dst_ref=ref,
            send_sem=send,
            recv_sem=receive,
            device_id=device(far[0]),
            device_id_type=MESH_ID,
        )
        sent.append(copy)
        return copy

    def neighbour_copy(turn, number):
        return pltpu.make_async_remote_copy(
            src_ref=fbuf.at[turn - 1, 0] if turn else nbuf.at[0],
            dst_ref=fbuf.at[turn - 1, number] if turn else nbuf.at[number],
            send_sem=nsend.at[turn],
            recv_sem=nrecv.at[turn],
            device_id=device(negated(slots[number])),
            device_id_type=MESH_ID,
        )

    def send_round(turn):
        far_first = sorted(range(1, len(slots)), key=lambda k: (-sum(map(abs, slots[k])), k))
        go([neighbour_copy(turn, number) for number in far_first])

    def wait_round(turn):
        others = pl.ds(1, len(slots) - 1)
        landed = fbuf.at[turn - 1, others] if turn else nbuf.at[others]
        every(landed, nsend.at[turn], nrecv.at[turn]).wait_recv()

    def away(offset):
        return sum(min(o, n - o) for o, n in zip(offset, counts))

    stages = {
        "near": (near, rbuf.at[0], ssend.at[0], srecv.at[0]),
        "far": (far, sbuf.at[0], ssend.at[1], srecv.at[1]),
        1: (whole, dbuf.at[0], ssend.at[2], srecv.at[2]),
        2: (whole, dbuf.at[1], ssend.at[3], srecv.at[3]),
    }

    def send_sum(stage, value):
        members, buffer, send, receive = stages[stage]
        buffer[0] = value
        for number in sorted(range(len(members)), key=lambda k: (-away(members[k]), k)):
            pltpu.make_async_remote_copy(
                src_ref=buffer.at[0],
                dst_ref=buffer.at[number + 1],
                send_sem=send,
                recv_sem=receive,
                device_id=device(negated(members[number])),
                device_id_type=MESH_ID,
            ).start()

    def wait_sum(stage):
        members, buffer, send, receive = stages[stage]
        every(buffer.at[pl.ds(1, len(members))], send, receive).wait_recv()
        total = buffer[...]
        while total.shape[0] > 1:
            half = total.shape[0] // 2
            total = total[:half] + total[half:]
        return total[0]

    def put(turn, vector):
        for c in range(3):
            for part in range(cap // 128):
                fbuf[turn - 1, 0, c, pl.ds(part, 1), :] = vector[
                    c : c + 1, part * 128 : part * 128 + 128
                ]

    def joined(ref, at, number, k):
        return jnp.concatenate(
            [ref[at, number, k, pl.ds(part, 1), :] for part in range(cap // 128)], axis=1
        )

    def mark(number, k):
        each = cap // 128
        parts = [divmod(k * each + part, 4) for part in range(each)]
        return jnp.concatenate([nbuf[number, a, pl.ds(b, 1), :] for a, b in parts], axis=1)

    def halo_copy(number, source, target, step):
        return pltpu.make_async_remote_copy(
            src_ref=source,
            dst_ref=target,
            send_sem=hsend.at[number],
            recv_sem=hrecv.at[number],
            device_id=device(negated(step)),
            device_id_type=MESH_ID,
        )

    corners_first = sorted(FLAT, key=lambda o: -abs(o[0]) - abs(o[1]))

    def halos(kind):
        parts, low, high, slot = KINDS[kind]
        (source_x, source_low, source_high, source_start, source_end), targets = (
            (block.at[pl.ds(parts[0], len(parts))], *packs[kind]),
            landing[kind],
        )
        more = -(-high * slot // size_y)
        spaces = (
            (source_x, targets[0], {-1: (size_x - low, low, 0), 1: (0, high, low)}),
            (source_low, targets[1], {-1: (low - 1, 1, 0), 0: (0, low, 1), 1: (0, 1, low + 1)}),
            (source_high, targets[2], {-1: (slot - 1, 1, 0), 0: (0, slot, 1), 1: (0, more, slot + 1)}),
        )
        copies = []
        for step_x, step_y in corners_first:
            if step_x or step_y:
                space = 0 if step_y == 0 else 1 if step_y < 0 else 2
                source, target, where = spaces[space]
                first, many, at = where[step_x]
                copies.append(
                    halo_copy(
                        4 * kind + space,
                        source.at[:, pl.ds(first, many)],
                        target.at[:, pl.ds(at, many)],
                        (step_x, step_y, 0),
                    )
                )
        for step_x, step_y in corners_first:
            for side, step_z in enumerate((-1, 1)):
                copies.append(
                    halo_copy(
                        4 * kind + 3,
                        (source_start, source_end)[side],
                        targets[3].at[side, FLAT.index((step_x, step_y))],
                        (step_x, step_y, step_z),
                    )
                )
        return copies

    def wait_halos(kind):
        for space, target in enumerate(landing[kind]):
            at = 4 * kind + space
            every(target, hsend.at[at], hrecv.at[at]).wait_recv()

    lane = lax.broadcasted_iota(jnp.int32, (size_y, size_z), 1)
    row = lax.broadcasted_iota(jnp.int32, (size_y, size_z), 0)

    def turned(value, by, axis):
        by %= value.shape[axis]
        return pltpu.roll(value, by, axis) if by else value

    def pack(kind):
        parts, low, high, slot = KINDS[kind]
        source_low, source_high, source_start, source_end = packs[kind]
        starts = [jnp.zeros((size_y, size_z), jnp.float32)] * 2
        ends = [jnp.zeros((size_y, size_z), jnp.float32)] * 2
        for i, c in enumerate(parts):
            tiles_low, tiles_high = [None] * low, [None] * slot
            for plane in range(size_x):
                own = block[c, plane]
                t, q = divmod(plane, size_y // low)
                moved = turned(own, low * (q + 1) - size_y, 0)
                tiles_low[t] = moved if q == 0 else jnp.where(row // low == q, moved, tiles_low[t])
                t, q = divmod(plane, size_y // slot)
                moved = turned(own, slot * q, 0)
                tiles_high[t] = moved if q == 0 else jnp.where(row // slot == q, moved, tiles_high[t])
                at = i * size_x + plane
                chain = plane % 2
                starts[chain] = jnp.where(
                    lane // low == at, turned(own, low * (at + 1) - size_z, 1), starts[chain]
                )
                ends[chain] = jnp.where(lane // slot == at, turned(own, slot * at, 1), ends[chain])
            for t in range(low):
                source_low[i, t] = tiles_low[t]
            for t in range(slot):
                source_high[i, t] = tiles_high[t]
        source_start[...] = jnp.where(lane // low % 2 == 0, starts[0], starts[1])
        source_end[...] = jnp.where(lane // slot % 2 == 0, ends[0], ends[1])

    def tall_of(down, own, up):
        moved = turned(own, LOW, 0)
        return jnp.where(row < LOW, down, moved), jnp.where(row < LOW, moved, up)

    def widen(kind):
        parts, low, high, slot = KINDS[kind]
        xbuf, below, above, zbuf = landing[kind]
        blank = 1.0 if kind else 0.0
        sides = {}
        for step_x in STEPS:
            for side in range(2):
                down, own, up = (zbuf[side, FLAT.index((step_x, step_y))] for step_y in (-1, 0, 1))
                sides[step_x, side] = tall_of(turned(down, LOW, 0), own, turned(up, LOW, 0))
        for x in range(-low, size_x + high):
            step_x = -1 if x < 0 else 0 if x < size_x else 1
            inner = x - step_x * size_x
            for i, c in enumerate(parts):
                own = block[c, x] if step_x == 0 else xbuf[i, x + low if step_x < 0 else x - size_x + low]
                t, q = divmod(inner, size_y // low)
                t = (0, t + 1, low + 1)[step_x + 1]
                down = turned(below[i, t], LOW - low * (q + 1), 0)
                t, q = divmod(inner, size_y // slot)
                t = (0, t + 1, t + slot + 1)[step_x + 1]
                up = turned(above[i, t], LOW - slot * q, 0)
                if low < LOW:
                    down = jnp.where(row >= LOW - low, down, blank)
                talls = tall_of(down, own, jnp.where(row < LOW + high, up, blank))
                at = i * size_x + inner
                for half in range(2):
                    moved = turned(talls[half], LOW, 1)
                    start = turned(sides[step_x, 0][half], LOW - low * (at + 1), 1)
                    end = turned(sides[step_x, 1][half], LOW - slot * at, 1)
                    if low < LOW:
                        start = jnp.where(lane >= LOW - low, start, blank)
                    left = jnp.where(lane < LOW, start, moved)
                    right = jnp.where(lane < LOW, moved, jnp.where(lane < LOW + high, end, blank))
                    if half:
                        left = jnp.where(row < LOW + high, left, blank)
                        right = jnp.where(row < LOW + high, right, blank)
                    if kind:
                        left, right = lax.rsqrt(left), lax.rsqrt(right)
                    rows = pl.ds(half * size_y, size_y)
                    fields[c, x + LOW, rows, pl.ds(0, size_z)] = left
                    fields[c, x + LOW, rows, pl.ds(size_z, size_z)] = right

    def tables(step_x, step_y, step_z):
        number = slots.index((step_x, step_y, step_z))
        cells = [mark(number, k) for k in range(3)]
        fours = [weights(mark(number, k + 3)) for k in range(3)]
        start, planes, first_row, rows, base = PATCHES[step_x, step_y]
        first = start // 8 * 8
        tall = round_up(start + planes - first, 8)
        tab_x = table(cells[0], fours[0], step_x, size_x, float(first), tall)
        tab_y = table(cells[1], fours[1], step_y, size_y, float(first_row), rows)
        return cells[2], fours[2], [
            tab_x[start - first + plane : start - first + plane + 1] * tab_y for plane in range(planes)
        ]

    def build_main(step_x, step_y):
        cell, four, products = tables(step_x, step_y, 0)
        start, planes, first_row, rows, base = PATCHES[step_x, step_y]
        for plane, product in enumerate(products):
            txy[pl.ds(base + plane * rows, rows), :] = product
        k = FLAT.index((step_x, step_y))
        if k:
            high, low = split(table(cell, four, 0, size_z, 0.0, lanes).T)
            thi[k], tlo[k] = high, low
            return
        high, low = split(table(cell, four, 0, size_z, 0.0, used))
        for ref, part in ((thi, high), (tlo, low)):
            ref[k, pl.ds(0, used), :] = part
            ref[k, pl.ds(used, lanes - used), :] = jnp.zeros((lanes - used, cap), jnp.bfloat16)

    def build_side(step_x, step_y, side):
        cell, four, products = tables(step_x, step_y, (-1, 1)[side])
        start, planes, first_row, rows, base = PATCHES[step_x, step_y]
        many = planes * rows
        high, low = split(jnp.concatenate(products, axis=0))
        azz[side, pl.ds(2 * base, many), :] = high
        azz[side, pl.ds(2 * base + many, many), :] = low
        k = FLAT.index((step_x, step_y))
        tzz[side, k] = table(cell, four, (-1, 1)[side], size_z, float(side * size_z), 8)

    own_planes = PATCHES[0, 0][1]
    own_rows = own_planes * TALL
    used = round_up(size_z + 5, 16)

    def interpolate(field):
        high, low = split(field.reshape(3 * own_rows, lanes))
        z_high, z_low = thi[0], tlo[0]
        part = dot_nn(high, z_high) + dot_nn(low, z_high) + dot_nn(high, z_low)
        plane = txy[pl.ds(0, own_rows), :]
        return jnp.concatenate(
            [
                jnp.sum(part[c * own_rows : (c + 1) * own_rows] * plane, axis=0, keepdims=True)
                for c in range(3)
            ],
            axis=0,
        )

    def spread_main(turn, step_x, step_y):
        start, planes, first_row, rows, base = PATCHES[step_x, step_y]
        number = slots.index((step_x, step_y, 0))
        k = FLAT.index((step_x, step_y))
        plane = txy[pl.ds(base, planes * rows), :]
        high, low = split(
            jnp.concatenate([plane * joined(fbuf, turn - 1, number, c) for c in range(3)], axis=0)
        )
        if k:
            dot, where = dot_nn, (k, slice(None), pl.ds(0, used))
        else:
            dot, where = dot_nt, (k, pl.ds(0, used), slice(None))
        z_high, z_low = thi[where], tlo[where]
        part = dot(high, z_high) + dot(low, z_high) + dot(high, z_low)
        part = part.reshape(3, planes, rows, used)
        if number == 0:
            for edge_plane in (0, WIDE - 1):
                grid[:, edge_plane] = jnp.zeros((3, TALL, lanes), jnp.float32)
            grid[:, pl.ds(start, planes), :, pl.ds(0, used)] = part
        else:
            grid[:, pl.ds(start, planes), pl.ds(first_row, rows), pl.ds(0, used)] += part

    def spread_side(turn, step_x, step_y, side):
        start, planes, first_row, rows, base = PATCHES[step_x, step_y]
        number = slots.index((step_x, step_y, (-1, 1)[side]))
        k = FLAT.index((step_x, step_y))
        many = planes * rows
        tab = tzz[side, k]
        pieces = [tab * joined(fbuf, turn - 1, number, c) for c in range(3)]
        high, low = split(jnp.concatenate(pieces + [jnp.zeros_like(tab)], axis=0))
        part = dot_nt(
            azz[side, pl.ds(2 * base, 2 * many), :], jnp.concatenate([high, low], axis=0)
        )
        part = (part[:many] + part[many:]).reshape(planes, rows, 64)
        where = (side, pl.ds(start, planes), pl.ds(first_row, rows), pl.ds(0, 64))
        if (step_x, step_y) == (0, 0):
            edge[where] = part
        else:
            edge[where] += part

    def finish_sides():
        inside = lax.broadcasted_iota(jnp.int32, (WIDE, TALL, size_z), 2) < 8
        for side in range(2):
            both = edge[side]
            both = both + turned(both, -32, 2)
            for c in range(3):
                part = jnp.where(inside, turned(both, -8 * c, 2), 0.0)
                grid[c, :, :, pl.ds(side * size_z, size_z)] += part

    def spread_rest(turn):
        wait_round(turn)
        for side in range(2):
            for edge_plane in (0, WIDE - 1):
                edge[side, edge_plane] = jnp.zeros((TALL, size_z), jnp.float32)
        for step_x, step_y in FLAT:
            for side in range(2):
                spread_side(turn, step_x, step_y, side)
        for step_x, step_y in FLAT:
            if step_x or step_y:
                spread_main(turn, step_x, step_y)
        finish_sides()

    def add(value, axis):
        return turned(value, -1, axis) + turned(value, 1, axis)

    def sub(value, axis):
        return turned(value, -1, axis) - turned(value, 1, axis)

    def respond():
        scale = fields[3]
        mx, my, mz = (scale * grid[c] for c in range(3))
        slope_y, slope_z = sub(my, 1), sub(mz, 2)
        sum_x = 2.0 * mx + add(mx, 1) + add(mx, 2)
        slope = slope_y + slope_z
        px = sum_x[2:] + sum_x[:-2] + slope[2:] - slope[:-2]
        slope_x = mx[2:] - mx[:-2]
        sum_y = (2.0 * my + add(my, 2))[1:-1] + my[2:] + my[:-2]
        tilt = slope_x + slope_z[1:-1]
        py = turned(sum_y + tilt, -1, 1) + turned(sum_y - tilt, 1, 1)
        sum_z = (2.0 * mz + add(mz, 1))[1:-1] + mz[2:] + mz[:-2]
        tilt = slope_x + slope_y[1:-1]
        pz = turned(sum_z + tilt, -1, 2) + turned(sum_z - tilt, 1, 2)
        half = scale[1:-1] * 0.5
        return jnp.stack(
            [half * (m[1:-1] + p * (1.0 / 12.0)) for m, p in ((mx, px), (my, py), (mz, pz))]
        )

    def apply(turn, vector):
        spread_rest(turn)
        return live * (interpolate(respond()) + stiffness * vector)

    left_half = lax.broadcasted_iota(jnp.int32, (1, 128), 1) < 64

    def partial_sums(residual, image):
        folded = []
        for other in (residual, image):
            line = jnp.sum(residual * other, axis=0, keepdims=True)
            total = line[:, :128]
            for at in range(128, cap, 128):
                total = total + line[:, at : at + 128]
            folded.append(total + turned(total, 64, 1))
        return jnp.where(left_half, folded[0], folded[1])

    def totals(tile):
        return (
            jnp.sum(jnp.where(left_half, tile, 0.0), axis=1, keepdims=True),
            jnp.sum(jnp.where(left_half, 0.0, tile), axis=1, keepdims=True),
        )

    loads[0].wait()
    pack(0)
    pl.semaphore_wait(barrier, len(peers))
    go(halos(0))
    loads[2].wait()
    loads[3].wait()
    each = cap // 128
    for k, size in enumerate(sizes):
        local = (cells_ref[pl.ds(k, 1), :] - me[k] * size).astype(jnp.float32)
        for values, at in ((local, k), (offsets_ref[pl.ds(k, 1), :], k + 3)):
            for part in range(each):
                a, b = divmod(at * each + part, 4)
                nbuf[0, a, pl.ds(b, 1), :] = values[:, part * 128 : part * 128 + 128]
    send_round(0)
    loads[1].wait()
    pack(1)
    go(halos(1))
    for load in loads[4:]:
        load.wait()
    target, stiffness = target_ref[...], stiffness_ref[...]
    live = (lax.broadcasted_iota(jnp.int32, (1, cap), 1) < count_ref[0]).astype(jnp.float32)
    build_main(0, 0)
    edge[...] = jnp.zeros_like(edge)
    grid[...] = jnp.zeros_like(grid)
    wait_halos(0)
    widen(0)
    base = live * (target - interpolate(fields[pl.ds(0, 3), pl.ds(1, own_planes)]))
    put(1, base)
    send_round(1)
    spread_main(1, 0, 0)
    wait_round(0)
    for step_x, step_y in FLAT:
        if step_x or step_y:
            build_main(step_x, step_y)
        build_side(step_x, step_y, 0)
        build_side(step_x, step_y, 1)
    wait_halos(1)
    widen(1)
    first = apply(1, base)
    send_sum("near", partial_sums(base, first))
    put(2, first)
    send_round(2)
    spread_main(2, 0, 0)
    send_sum("far", wait_sum("near"))
    second = apply(2, first)
    put(3, second)
    send_round(3)
    spread_main(3, 0, 0)
    norm, product = totals(wait_sum("far"))
    alpha = norm / product
    answer = alpha * base
    residual, image = base - alpha * first, first - alpha * second
    send_sum(1, partial_sums(residual, image))
    third = apply(3, second)
    again = second - alpha * third
    norm_before, alpha_before = norm, alpha
    norm, product = totals(wait_sum(1))
    ratio = norm / norm_before
    alpha = norm / (product - ratio * norm / alpha_before)
    direction = residual + ratio * base
    answer = answer + alpha * direction
    residual, image = (
        residual - alpha * (image + ratio * first),
        image - alpha * (again + ratio * second),
    )
    send_sum(2, partial_sums(residual, image))
    norm_before, alpha_before = norm, alpha
    norm, product = totals(wait_sum(2))
    ratio = norm / norm_before
    alpha = norm / (product - ratio * norm / alpha_before)
    out[...] = answer + alpha * (residual + ratio * direction)
    for copy in sent:
        copy.wait_send()


def body(mesh_counts, density, base_velocity, cells, offsets, target, stiffness, counts):
    sizes = density.shape
    size_x, size_y, size_z = sizes
    cap = cells.shape[1]
    assert sizes == (8, 8, 128) and min(mesh_counts) > 2
    lanes = 2 * size_z
    number, flat = 27, 9
    turns = ITERS + 1
    halo_shapes = []
    for parts, low, high, slot in KINDS:
        more = -(-high * slot // size_y)
        halo_shapes += [(len(parts), low), (len(parts), slot), (), (), (len(parts), low + high)]
        halo_shapes += [(len(parts), low + 2), (len(parts), slot + 1 + more), (2, flat)]
    near, far = mesh_counts[1] * mesh_counts[2], mesh_counts[0]
    return pl.pallas_call(
        functools.partial(kernel, mesh_counts, sizes),
        out_shape=jax.ShapeDtypeStruct((3, cap), jnp.float32),
        in_specs=[pl.BlockSpec(memory_space=pltpu.HBM)] * 7,
        out_specs=pl.BlockSpec(memory_space=pltpu.VMEM),
        scratch_shapes=[
            pltpu.VMEM((4, size_x, size_y, size_z), jnp.float32),
            pltpu.VMEM((3, cap), jnp.int32),
            pltpu.VMEM((3, cap), jnp.float32),
            pltpu.VMEM((3, cap), jnp.float32),
            pltpu.VMEM((1, cap), jnp.float32),
            pltpu.SMEM((1,), jnp.int32),
            pltpu.VMEM((4, WIDE, TALL, lanes), jnp.float32),
            *[pltpu.VMEM(shape + (size_y, size_z), jnp.float32) for shape in halo_shapes],
            pltpu.VMEM((number, 3 * (cap // 256), 4, 128), jnp.float32),
            pltpu.VMEM((ITERS, number, 3, cap // 128, 128), jnp.float32),
            pltpu.VMEM((1, near, 1, 128), jnp.float32),
            pltpu.VMEM((1, far, 1, 128), jnp.float32),
            pltpu.VMEM((2, near * far, 1, 128), jnp.float32),
            pltpu.VMEM((PATCH_ROWS, cap), jnp.float32),
            pltpu.VMEM((flat, lanes, cap), jnp.bfloat16),
            pltpu.VMEM((flat, lanes, cap), jnp.bfloat16),
            pltpu.VMEM((2, 2 * PATCH_ROWS, cap), jnp.bfloat16),
            pltpu.VMEM((2, flat, 8, cap), jnp.float32),
            pltpu.VMEM((2, WIDE, TALL, size_z), jnp.float32),
            pltpu.VMEM((3, WIDE, TALL, lanes), jnp.float32),
            pltpu.SemaphoreType.DMA((7,)),
            pltpu.SemaphoreType.DMA((turns,)),
            pltpu.SemaphoreType.DMA((turns,)),
            pltpu.SemaphoreType.DMA((4,)),
            pltpu.SemaphoreType.DMA((4,)),
            pltpu.SemaphoreType.DMA((8,)),
            pltpu.SemaphoreType.DMA((8,)),
        ],
        compiler_params=pltpu.CompilerParams(
            collective_id=0, has_side_effects=True, vmem_limit_bytes=60 * 1024 * 1024
        ),
    )(density, base_velocity, cells, offsets, target, stiffness[None], counts)


def solution(mesh):
    return jax.shard_map(
        functools.partial(body, tuple(mesh.shape[name] for name in AXES)),
        mesh=mesh,
        in_specs=(
            P("gx", "gy", "gz"),
            P(None, "gx", "gy", "gz"),
            P(None, ("gx", "gy", "gz")),
            P(None, ("gx", "gy", "gz")),
            P(None, ("gx", "gy", "gz")),
            P(("gx", "gy", "gz")),
            P(("gx", "gy", "gz")),
        ),
        out_specs=P(None, ("gx", "gy", "gz")),
        check_vma=False,
    )
```
